32 devices in a mesh: crops: 1, rows: 16 (over z, y, core), cols: 2 (over x).
Axes of the slice: x: 2, y: 2, z: 4, core: 2. Of those that a mesh axis runs over, the one named last changes fastest.
Arguments:
- family_representation: float32 [128, 256, 256], P(('crops', 'rows'), 'cols'), may hold values from -6 to 6
- family_keep_flags: int32 [128, 256], P(('crops', 'rows'), 'cols'), may hold values 0 or 1
- amino_presence: int32 [256], P('crops'), may hold values 0 or 1
- contact_embedding: float32 [256, 256, 128], P(('crops', 'rows'), 'cols'), may hold values from -6 to 6
- couple_lhs_weights: bfloat16 [256, 32], replicated, may hold values from -0.375 to 0.375
- couple_rhs_weights: bfloat16 [256, 32], replicated, may hold values from -0.375 to 0.375
- pairwise_final_matrix: bfloat16 [1024, 128], replicated, may hold values from -1.5 to 1.5
- edge_source_matrix: bfloat16 [128, 256], replicated, may hold values from -0.5 to 0.5
- edge_target_matrix: bfloat16 [128, 256], replicated, may hold values from -0.5 to 0.5
- edge_final_sigmoid_matrix: bfloat16 [128, 128], replicated, may hold values from -0.5 to 0.5
- edge_final_matrix: bfloat16 [128, 128], replicated, may hold values from -0.5 to 0.5
- feedforward_expand_matrix: bfloat16 [128, 512], replicated, may hold values from -0.5 to 0.5
- feedforward_shrink_matrix: bfloat16 [512, 128], replicated, may hold values from -0.25 to 0.25
Outputs:
- pair_out: float32 [256, 256, 128], P(('crops', 'rows'), 'cols')
The draws below stay inside these ranges and needn't reach their ends.
All inputs are finite; a program needn't handle non-finite values. No bound on the sum of `family_keep_flags` on one device may be relied on, other than what follows from the above.
Results may differ from the reference program's by a relative error of at most 0.0053.
Values may be sent and summed in bfloat16 or wider, within the bound.
No kernel may reach another device: no remote copies, remote signals or barrier semaphores. Data moves between devices by JAX's collectives and lax.ppermute only.
A program may use at most 64 MiB of HBM per device.

```python
import jax
import jax.numpy as jnp
from jax import lax

FAMILY_FEATS = 256
OPM_CHANS = 32
CZ = 128
CT = 128
CH = 512
FAMILY_ENTRIES = 128
CRAFT_SPAN = 256


def set_ends(drawn, rng, low, high):
    place = [jax.random.randint(jax.random.fold_in(rng, axis), (), 0, length) for axis, length in enumerate(drawn.shape)]
    main_axis = drawn.shape.index(max(drawn.shape))
    neighbour = place[:main_axis] + [(place[main_axis] + 1) % drawn.shape[main_axis]] + place[main_axis + 1:]
    return drawn.at[tuple(place)].set(low).at[tuple(neighbour)].set(high)


def level_of(key, extent, pieces, least, top_value):
    gain, own = 1.0, jax.random.fold_in(key, 6)
    for position, shards_of in pieces:
        draws = jnp.exp(jax.random.uniform(jax.random.fold_in(own, position), (shards_of,), jnp.float32, least / len(pieces), top_value / len(pieces)))
        gain = gain * jnp.repeat(draws, extent[position] // shards_of).reshape([-1 if axis == position else 1 for axis in range(len(extent))])
    return gain


def gaussian(own_key, shape, scale, reach, cuts=(), held_as=jnp.bfloat16):
    loudness = level_of(own_key, shape, cuts, -0.22, 0.18) if cuts else 1.0
    values = jax.random.normal(own_key, shape, jnp.float32) * scale * loudness
    return jnp.minimum(jnp.maximum(values, -reach), reach).astype(held_as)


def setup_inputs(seed: int = 0, part: int = 0) -> dict:
    key_of = jax.random.split(jax.random.key(seed), 14)
    part_splits = jax.random.split(jax.random.fold_in(key_of[13], part), 14)
    return {
        "family_representation": gaussian(part_splits[0], (FAMILY_ENTRIES, CRAFT_SPAN, FAMILY_FEATS), 1.0, 6.0, ((0, 16), (1, 2)), jnp.float32),
        "family_keep_flags": set_ends((jax.random.randint(part_splits[1], (FAMILY_ENTRIES, CRAFT_SPAN), 0, 4) < 3).astype(jnp.int32), jax.random.fold_in(part_splits[1], 1), 0, 1),
        "amino_presence": set_ends((jax.random.randint(part_splits[2], (CRAFT_SPAN,), 0, 16) < 15).astype(jnp.int32), jax.random.fold_in(part_splits[2], 1), 0, 1),
        "contact_embedding": gaussian(part_splits[3], (CRAFT_SPAN, CRAFT_SPAN, CZ), 1.0, 6.0, ((0, 16), (1, 2)), jnp.float32),
        "couple_lhs_weights": gaussian(key_of[4], (FAMILY_FEATS, OPM_CHANS), FAMILY_FEATS ** -0.5, 0.375),
        "couple_rhs_weights": gaussian(key_of[5], (FAMILY_FEATS, OPM_CHANS), FAMILY_FEATS ** -0.5, 0.375),
        "pairwise_final_matrix": gaussian(key_of[6], (OPM_CHANS * OPM_CHANS, CZ), (OPM_CHANS * OPM_CHANS // 64) ** -0.5, 1.5),
        "edge_source_matrix": gaussian(key_of[7], (CZ, 2 * CT), CZ ** -0.5, 0.5),
        "edge_target_matrix": gaussian(key_of[8], (CZ, 2 * CT), CZ ** -0.5, 0.5),
        "edge_final_sigmoid_matrix": gaussian(key_of[9], (CZ, CZ), CZ ** -0.5, 0.5),
        "edge_final_matrix": gaussian(key_of[10], (CT, CZ), CT ** -0.5, 0.5),
        "feedforward_expand_matrix": gaussian(key_of[11], (CZ, CH), CZ ** -0.5, 0.5),
        "feedforward_shrink_matrix": gaussian(key_of[12], (CH, CZ), CH ** -0.5, 0.25),
    }


epsilon = 1e-05

def normalise_features_step(values, reduce_axis):
    mean = lax.optimization_barrier(jnp.mean(values, axis=reduce_axis, keepdims=True))
    centred = values - mean
    spread = lax.optimization_barrier(jnp.mean(centred * centred, axis=reduce_axis, keepdims=True))
    return centred * lax.rsqrt(spread + epsilon)

def reduced_numeric_kind(values):
    return lax.optimization_barrier(values.astype(jnp.bfloat16)).astype(jnp.float32)

def growth_multiple(values):
    return values.astype(jnp.float32)

def reference(family_representation, family_keep_flags, amino_presence, contact_embedding, couple_lhs_weights, couple_rhs_weights, pairwise_final_matrix, edge_source_matrix, edge_target_matrix, edge_final_sigmoid_matrix, edge_final_matrix, feedforward_expand_matrix, feedforward_shrink_matrix):
    family_tally = family_representation.shape[0]
    polymer_extent = family_representation.shape[1]
    intermediate_breadth = couple_lhs_weights.shape[1]
    residue_float_mask = amino_presence.astype(jnp.float32)
    retained_family_entries = family_keep_flags.astype(jnp.float32) * residue_float_mask[None, :]
    rescaled_family_rep = reduced_numeric_kind(normalise_features_step(family_representation.astype(jnp.float32), -1))
    family_lhs_mapped = reduced_numeric_kind(jnp.einsum('ohp,pd->ohd', rescaled_family_rep, growth_multiple(couple_lhs_weights)) * retained_family_entries[:, :, None])
    family_rhs_mapped = reduced_numeric_kind(jnp.einsum('ohp,pd->ohd', rescaled_family_rep, growth_multiple(couple_rhs_weights)) * retained_family_entries[:, :, None])
    portion_number = 8
    port_portion_group = family_lhs_mapped.reshape(family_tally, polymer_extent // portion_number, portion_number, intermediate_breadth).transpose(1, 0, 2, 3)
    live_blocks = retained_family_entries.reshape(family_tally, polymer_extent // portion_number, portion_number).transpose(1, 0, 2)
    out_weight = growth_multiple(pairwise_final_matrix)

    def outer_block(item):
        port_segments, lives = item
        averaged_tensor_contraction = jnp.einsum('lyj,lnx->ynjx', port_segments, family_rhs_mapped)
        counts = jnp.einsum('si,sj->ij', lives, retained_family_entries)
        mean = reduced_numeric_kind(averaged_tensor_contraction / jnp.maximum(counts, 1.0)[:, :, None, None])
        flat = mean.reshape(portion_number * polymer_extent, intermediate_breadth * intermediate_breadth)
        return jnp.dot(flat, out_weight).reshape(portion_number, polymer_extent, -1)
    update = lax.map(outer_block, (port_portion_group, live_blocks)).reshape(polymer_extent, polymer_extent, -1)
    first = contact_embedding + update
    pair_normed = reduced_numeric_kind(normalise_features_step(first, -1))
    pair_live = residue_float_mask[:, None] * residue_float_mask[None, :]
    left_raw = jnp.einsum('ijz,zc->cij', pair_normed, growth_multiple(edge_source_matrix))
    channels = left_raw.shape[0] // 2
    left_panel = reduced_numeric_kind(left_raw[:channels] * jax.nn.sigmoid(left_raw[channels:]) * pair_live[None])
    right_raw = jnp.einsum('ijz,zc->cij', pair_normed, growth_multiple(edge_target_matrix))
    right_panel = reduced_numeric_kind(right_raw[:channels] * jax.nn.sigmoid(right_raw[channels:]) * pair_live[None])
    product = reduced_numeric_kind(jnp.einsum('cik,cjk->cij', left_panel, right_panel))
    mixed = reduced_numeric_kind(normalise_features_step(product, 0))
    gate = jax.nn.sigmoid(jnp.einsum('ijz,zy->ijy', pair_normed, growth_multiple(edge_final_sigmoid_matrix)))
    second = first + gate * jnp.einsum('cij,cz->ijz', mixed, growth_multiple(edge_final_matrix))
    first_weight = growth_multiple(feedforward_expand_matrix)
    second_weight = growth_multiple(feedforward_shrink_matrix)

    def finish(row_indices):
        normed_rows = reduced_numeric_kind(normalise_features_step(row_indices, -1))
        hidden = reduced_numeric_kind(jax.nn.relu(jnp.dot(normed_rows, first_weight)))
        return row_indices + jnp.dot(hidden, second_weight)
    result = lax.map(finish, second.reshape(polymer_extent // portion_number, portion_number, polymer_extent, -1))
    return result.reshape(polymer_extent, polymer_extent, -1)
```

```python
import functools

import jax
import jax.numpy as jnp
from jax import lax
from jax.experimental import pallas as pl
from jax.experimental.pallas import tpu as pltpu
from jax.sharding import PartitionSpec as P

EPS = 1e-05
F32 = jnp.float32
BF16 = jnp.bfloat16
TILE = 16
LANES = 128
VMEM = pl.BlockSpec(memory_space=pltpu.VMEM)


def dot(a, b):
    return lax.dot_general(a, b, (((1,), (0,)), ((), ())), preferred_element_type=F32)


def dot_nt(a, b):
    return lax.dot_general(a, b, (((1,), (1,)), ((), ())), preferred_element_type=F32)


def sigmoid(x):
    return 0.5 * jnp.tanh(0.5 * x) + 0.5


def call(kernel, out_shape, scratch, name):
    def run(*args):
        return pl.pallas_call(
            kernel,
            out_shape=out_shape,
            in_specs=[VMEM] * len(args),
            out_specs=jax.tree.map(lambda _: VMEM, out_shape),
            scratch_shapes=scratch,
            name=name,
        )(*args)

    return run


def project_kernel(fam_ref, keep_ref, pres_ref, wl_ref, wr_ref, right_ref, left_ref, nf, rs, *, tile_rows):
    seqs, cols, feats = fam_ref.shape
    chans = wl_ref.shape[1]
    col = lax.axis_index("cols")
    live = (keep_ref[...] * pres_ref[pl.ds(col, 1), :]).astype(F32)
    live_t = jnp.concatenate([live, jnp.zeros((LANES - seqs, cols), F32)], 0).T
    wr_t = wr_ref[...].astype(F32).T.astype(BF16)
    for s in range(seqs):
        v = fam_ref[s]
        centred = v - jnp.mean(v, -1, keepdims=True)
        spread = jnp.mean(centred * centred, -1, keepdims=True)
        n = centred * (lax.rsqrt(spread + EPS) * live_t[:, s : s + 1])
        for h in range(feats // LANES):
            nf[h, pl.ds(s * cols, cols), :] = n[:, h * LANES : (h + 1) * LANES]
        rs[pl.ds(s, chans, stride=seqs), :] = dot_nt(wr_t, n.astype(BF16))
    right_ref[0 : chans * seqs, :] = rs[...].astype(BF16)
    live_tile = jnp.concatenate([live, jnp.zeros((TILE - seqs, cols), F32)], 0).astype(BF16)
    right_ref[chans * seqs : chans * seqs + TILE, :] = live_tile
    per = LANES // chans
    groups = tile_rows // per
    pieces = cols // tile_rows
    wl = wl_ref[...].astype(F32)
    acc = None
    for i4 in range(per):
        parts = []
        if i4:
            parts.append(jnp.zeros((feats, i4 * chans), F32))
        parts.append(wl)
        if i4 < per - 1:
            parts.append(jnp.zeros((feats, (per - 1 - i4) * chans), F32))
        w = jnp.concatenate(parts, 1).astype(BF16)
        rows = [
            jnp.concatenate(
                [nf[h, pl.ds(pq * per + i4, seqs, stride=cols), :] for h in range(feats // LANES)], 1
            )
            for pq in range(pieces * groups)
        ]
        part = dot(jnp.concatenate(rows, 0).astype(BF16), w)
        acc = part if acc is None else acc + part
    block = groups * seqs
    for p in range(pieces):
        left_ref[p, 0:block, :] = acc[p * block : (p + 1) * block].astype(BF16)
        left_ref[p, block : block + TILE, :] = live_tile


def pair_kernel(
    right0_ref, right1_ref, left_ref, contact_ref, pres_ref, wo_ref, wp_ref,
    first_ref, gate_ref, panel_ref,
    o_scr, cnt_scr, pan_scr,
    *, seqs, radix, tile_rows, chans,
):
    tiles = right0_ref.shape[1] // TILE - 1
    half = right0_ref.shape[0]
    blocks = 2 * half
    cols = right0_ref.shape[2]
    feats = first_ref.shape[1]
    width = pan_scr.shape[1] // tile_rows
    pack = TILE // seqs
    per = LANES // chans
    groups = tile_rows // per
    row = lax.axis_index("rows")
    col = lax.axis_index("cols")
    z, y, c = row // 4, (row // 2) % 2, row % 2

    def source(b):
        cz, cy, cc = b % radix, (b // radix) % 2, b // (2 * radix)
        return lax.rem(z + radix - cz, radix) * 4 + (y ^ cy) * 2 + (c ^ cc)

    def right(b, t):
        ref = right0_ref if b < half else right1_ref
        return ref[b % half, t * TILE : (t + 1) * TILE, :]

    lefts = [left_ref[source(b)].astype(F32) for b in range(blocks)]
    block = groups * seqs
    live_l = jnp.concatenate([v[block : block + seqs] for v in lefts], 0).T.astype(BF16)
    live_r = jnp.concatenate([right(b, tiles).astype(F32)[:seqs] for b in range(blocks)], 0).astype(BF16)
    cnt_scr[...] = dot(live_l, live_r)
    start = lax.rem(row * tile_rows, cols)
    inv = 1.0 / jnp.maximum(cnt_scr[pl.ds(pl.multiple_of(start, 8), tile_rows), :], 1.0)
    zero = jnp.zeros((seqs, LANES), F32)
    ops = []
    for d2 in range(pack):
        for q in range(groups):
            rows = []
            for v in lefts:
                rows += [v[q * seqs : (q + 1) * seqs] if k == d2 else zero for k in range(pack)]
            ops.append(jnp.concatenate(rows, 0).T.astype(BF16))
    a_ext = jnp.concatenate(ops, 0)

    for t in range(0, tiles, 2):
        rhs = jnp.concatenate(
            [jnp.concatenate([right(b, u) for b in range(blocks)], 0) for u in (t, t + 1)], 1
        )
        out = dot(a_ext, rhs)
        for k in range(2):
            for d2 in range(pack):
                for i in range(tile_rows):
                    at = (d2 * tile_rows + i) * chans
                    val = out[at : at + chans, k * cols : (k + 1) * cols] * inv[i : i + 1]
                    d = (t + k) * pack + d2
                    o_scr[i, d * chans : (d + 1) * chans, :] = val.astype(BF16)

    w_o = wo_ref[...]
    w_p = wp_ref[...]
    live_j = pres_ref[pl.ds(col, 1), :].astype(F32)
    live_i = pres_ref[pl.ds(lax.div(row * tile_rows, cols), 1), :].astype(F32)
    cnt_scr[0:LANES, :] = jnp.broadcast_to(live_i, (LANES, cols)).T
    live_rows = cnt_scr[pl.ds(pl.multiple_of(start, 8), tile_rows), :]
    for i in range(0, tile_rows, 2):
        upd = dot(w_o, jnp.concatenate([o_scr[i], o_scr[i + 1]], 1))
        normed = []
        for k in range(2):
            first = contact_ref[i + k] + upd[:, k * cols : (k + 1) * cols]
            first_ref[i + k] = first
            centred = first - jnp.mean(first, 0, keepdims=True)
            spread = jnp.mean(centred * centred, 0, keepdims=True)
            normed.append((centred * lax.rsqrt(spread + EPS)).astype(BF16))
        raw = dot(w_p, jnp.concatenate(normed, 1))
        for k in range(2):
            live = live_rows[i + k : i + k + 1] * live_j
            part = raw[:, k * cols : (k + 1) * cols]
            for side in range(2):
                at = side * 2 * width
                val = part[at : at + width] * sigmoid(part[at + width : at + 2 * width]) * live
                pan_scr[side, pl.ds(i + k, width, stride=tile_rows), :] = val
            gate_ref[i + k] = sigmoid(part[4 * width : 4 * width + feats])
    for ch in range(width):
        for side in range(2):
            panel_ref[ch, side] = pan_scr[side, ch * tile_rows : (ch + 1) * tile_rows, :].astype(BF16)


def triangle_kernel(recv_ref, out_ref, *, n_rows, n_cols):
    own = recv_ref.shape[1]
    tile_rows, cols = recv_ref.shape[3:]
    for ch in range(own):
        sides = [
            jnp.concatenate(
                [
                    jnp.concatenate([recv_ref[r * n_cols + x, ch, side] for r in range(n_rows)], 0)
                    for x in range(n_cols)
                ],
                1,
            )
            for side in range(2)
        ]
        prod = dot_nt(sides[0], sides[1]).astype(BF16)
        for r in range(n_rows):
            for x in range(n_cols):
                out_ref[r * n_cols + x, ch] = prod[
                    r * tile_rows : (r + 1) * tile_rows, x * cols : (x + 1) * cols
                ]


def finish_kernel(prod_ref, first_ref, gate_ref, we_ref, w1_ref, w2_ref, out_ref, mix):
    chans, tile_rows, cols = prod_ref.shape
    total = jnp.zeros((tile_rows, cols), F32)
    for ch in range(chans):
        total = total + prod_ref[ch].astype(F32)
    mean = total * (1.0 / chans)
    square = jnp.zeros((tile_rows, cols), F32)
    for ch in range(chans):
        centred = prod_ref[ch].astype(F32) - mean
        square = square + centred * centred
    scale = lax.rsqrt(square * (1.0 / chans) + EPS)
    for ch in range(chans):
        mix[ch * tile_rows : (ch + 1) * tile_rows, :] = (prod_ref[ch].astype(F32) - mean) * scale
    w_e, w_1, w_2 = we_ref[...], w1_ref[...], w2_ref[...]
    for i in range(0, tile_rows, 2):
        mixed = jnp.concatenate(
            [mix[pl.ds(i + k, chans, stride=tile_rows), :].astype(BF16) for k in range(2)], 1
        )
        proj = dot(w_e, mixed)
        seconds, normed = [], []
        for k in range(2):
            second = first_ref[i + k] + gate_ref[i + k] * proj[:, k * cols : (k + 1) * cols]
            centred = second - jnp.mean(second, 0, keepdims=True)
            spread = jnp.mean(centred * centred, 0, keepdims=True)
            seconds.append(second)
            normed.append((centred * lax.rsqrt(spread + EPS)).astype(BF16))
        hidden = jnp.maximum(dot(w_1, jnp.concatenate(normed, 1)), 0.0).astype(BF16)
        out = dot(w_2, hidden)
        for k in range(2):
            out_ref[i + k] = (seconds[k] + out[:, k * cols : (k + 1) * cols]).T


def on_device(
    family_representation,
    family_keep_flags,
    amino_presence,
    contact_embedding,
    couple_lhs_weights,
    couple_rhs_weights,
    pairwise_final_matrix,
    edge_source_matrix,
    edge_target_matrix,
    edge_final_sigmoid_matrix,
    edge_final_matrix,
    feedforward_expand_matrix,
    feedforward_shrink_matrix,
):
    seqs, cols, feats = family_representation.shape
    tile_rows, _, pair_feats = contact_embedding.shape
    n_rows = lax.axis_size("rows")
    n_cols = lax.axis_size("cols")
    chans = couple_lhs_weights.shape[1]
    width = edge_source_matrix.shape[1] // 2
    devices = n_rows * n_cols
    radix = n_rows // 4
    pieces = cols // tile_rows
    col = lax.axis_index("cols")
    presence = amino_presence.reshape(n_cols, cols)
    shape = jax.ShapeDtypeStruct

    right_rows = chans * seqs + TILE
    left_rows = tile_rows * chans * seqs // LANES + TILE
    right, left = call(
        functools.partial(project_kernel, tile_rows=tile_rows),
        (shape((right_rows, cols), BF16), shape((pieces, left_rows, LANES), BF16)),
        [pltpu.VMEM((feats // LANES, seqs * cols, LANES), F32), pltpu.VMEM((chans * seqs, cols), F32)],
        "project",
    )(family_representation, family_keep_flags, presence, couple_lhs_weights, couple_rhs_weights)

    left_wide = jnp.zeros((n_cols, pieces, left_rows, LANES), BF16)
    left_wide = lax.dynamic_update_slice_in_dim(left_wide, left[None], col, 0)
    for k in range(1, n_cols):
        got = lax.ppermute(left, "cols", [(i, (i + k) % n_cols) for i in range(n_cols)])
        left_wide = lax.dynamic_update_slice_in_dim(left_wide, got[None], (col + n_cols - k) % n_cols, 0)
    blocks = [right]
    for k in range(1, radix):
        blocks.append(lax.ppermute(right, "rows", [(i, (i + 4 * k) % n_rows) for i in range(n_rows)]))
    right_z = jnp.stack(blocks)
    right_y = lax.ppermute(right_z, "rows", [(i, i ^ 2) for i in range(n_rows)])
    left_all = lax.all_to_all(
        left_wide.reshape(n_rows, left_rows, LANES), "rows", split_axis=0, concat_axis=0, tiled=True
    )
    right0 = jnp.concatenate([right_z, right_y], 0)
    right1 = lax.ppermute(right0, "rows", [(i, i ^ 1) for i in range(n_rows)])

    contact_t = contact_embedding.transpose(0, 2, 1)
    w_o = pairwise_final_matrix.reshape(chans, chans, pair_feats).transpose(2, 1, 0).reshape(pair_feats, chans * chans)
    w_p = jnp.concatenate([edge_source_matrix, edge_target_matrix, edge_final_sigmoid_matrix], 1).T
    pair = shape((tile_rows, pair_feats, cols), F32)
    first, gate, panels = call(
        functools.partial(pair_kernel, seqs=seqs, radix=radix, tile_rows=tile_rows, chans=chans),
        (pair, pair, shape((width, 2, tile_rows, cols), BF16)),
        [
            pltpu.VMEM((tile_rows, chans * chans, cols), BF16),
            pltpu.VMEM((LANES, cols), F32),
            pltpu.VMEM((2, width * tile_rows, cols), F32),
        ],
        "pair",
    )(right0, right1, left_all, contact_t, presence, w_o, w_p)

    panels = lax.all_to_all(
        panels.reshape(devices, width // devices, 2, tile_rows, cols),
        ("rows", "cols"), split_axis=0, concat_axis=0, tiled=True,
    )
    product = call(
        functools.partial(triangle_kernel, n_rows=n_rows, n_cols=n_cols),
        shape((devices, width // devices, tile_rows, cols), BF16),
        [],
        "triangle",
    )(panels)
    product = lax.all_to_all(product, ("rows", "cols"), split_axis=0, concat_axis=0, tiled=True)
    return call(
        finish_kernel,
        shape((tile_rows, cols, pair_feats), F32),
        [pltpu.VMEM((width * tile_rows, cols), F32)],
        "finish",
    )(
        product.reshape(width, tile_rows, cols), first, gate,
        edge_final_matrix.T, feedforward_expand_matrix.T, feedforward_shrink_matrix.T,
    )


def solution(mesh):
    tiles = P(("crops", "rows"), "cols", None)
    in_specs = (tiles, P(("crops", "rows"), "cols"), P("crops"), tiles) + (P(),) * 9
    return jax.shard_map(on_device, mesh=mesh, in_specs=in_specs, out_specs=tiles, check_vma=False)
```

```python
import functools

import jax
import jax.numpy as jnp
from jax import lax
from jax.experimental import pallas as pl
from jax.experimental.pallas import tpu as pltpu
from jax.sharding import PartitionSpec as P

EPS = 1e-05
F32 = jnp.float32
BF16 = jnp.bfloat16
TILE = 16
LANES = 128
VMEM = pl.BlockSpec(memory_space=pltpu.VMEM)


def dot(a, b):
    return lax.dot_general(a, b, (((1,), (0,)), ((), ())), preferred_element_type=F32)


def dot_nt(a, b):
    return lax.dot_general(a, b, (((1,), (1,)), ((), ())), preferred_element_type=F32)


def sigmoid(x):
    return 0.5 * jnp.tanh(0.5 * x) + 0.5


def call(kernel, out_shape, scratch, name):
    def run(*args):
        return pl.pallas_call(
            kernel,
            out_shape=out_shape,
            in_specs=[VMEM] * len(args),
            out_specs=jax.tree.map(lambda _: VMEM, out_shape),
            scratch_shapes=scratch,
            name=name,
        )(*args)

    return run


def project_kernel(fam_ref, keep_ref, pres_ref, wl_ref, wr_ref, right_ref, left_ref, nf, rs, *, tile_rows):
    seqs, cols, feats = fam_ref.shape
    chans = wl_ref.shape[0]
    col = lax.axis_index("cols")
    live = (keep_ref[...] * pres_ref[pl.ds(col, 1), :]).astype(F32)
    live_t = jnp.concatenate([live, jnp.zeros((LANES - seqs, cols), F32)], 0).T
    wr_t = wr_ref[...]
    for s in range(seqs):
        v = fam_ref[s]
        centred = v - jnp.mean(v, -1, keepdims=True)
        spread = jnp.mean(centred * centred, -1, keepdims=True)
        n = centred * (lax.rsqrt(spread + EPS) * live_t[:, s : s + 1])
        for h in range(feats // LANES):
            nf[h, pl.ds(s * cols, cols), :] = n[:, h * LANES : (h + 1) * LANES]
        rs[pl.ds(s, chans, stride=seqs), :] = dot_nt(wr_t, n.astype(BF16))
    right_ref[0 : chans * seqs, :] = rs[...].astype(BF16)
    live_tile = jnp.concatenate([live, jnp.zeros((TILE - seqs, cols), F32)], 0).astype(BF16)
    right_ref[chans * seqs : chans * seqs + TILE, :] = live_tile
    per = LANES // chans
    groups = tile_rows // per
    pieces = cols // tile_rows
    wl = wl_ref[...].astype(F32).T
    acc = None
    for i4 in range(per):
        parts = []
        if i4:
            parts.append(jnp.zeros((feats, i4 * chans), F32))
        parts.append(wl)
        if i4 < per - 1:
            parts.append(jnp.zeros((feats, (per - 1 - i4) * chans), F32))
        w = jnp.concatenate(parts, 1).astype(BF16)
        rows = [
            jnp.concatenate(
                [nf[h, pl.ds(pq * per + i4, seqs, stride=cols), :] for h in range(feats // LANES)], 1
            )
            for pq in range(pieces * groups)
        ]
        part = dot(jnp.concatenate(rows, 0).astype(BF16), w)
        acc = part if acc is None else acc + part
    block = groups * seqs
    for p in range(pieces):
        left_ref[p, 0:block, :] = acc[p * block : (p + 1) * block].astype(BF16)
        left_ref[p, block : block + TILE, :] = live_tile


def pair_kernel(
    right0_ref, right1_ref, left0_ref, left1_ref, contact_ref, pres_ref, wo_ref, wp_ref,
    first_ref, gate_ref, panel_ref,
    o_scr, cnt_scr, pan_scr,
    *, seqs, tile_rows, chans,
):
    tiles = right0_ref.shape[1] // TILE - 1
    half = right0_ref.shape[0]
    blocks = 2 * half
    cols = right0_ref.shape[2]
    feats = first_ref.shape[1]
    width = pan_scr.shape[1] // tile_rows
    pack = TILE // seqs
    per = LANES // chans
    groups = tile_rows // per
    row = lax.axis_index("rows")
    col = lax.axis_index("cols")
    def right(b, t):
        ref = right0_ref if b < half else right1_ref
        return ref[b % half, t * TILE : (t + 1) * TILE, :]

    lefts = [ref[b].astype(F32) for ref in (left0_ref, left1_ref) for b in range(half)]
    block = groups * seqs
    live_l = jnp.concatenate([v[block : block + seqs] for v in lefts], 0).T.astype(BF16)
    live_r = jnp.concatenate([right(b, tiles).astype(F32)[:seqs] for b in range(blocks)], 0).astype(BF16)
    cnt_scr[...] = dot(live_l, live_r)
    start = lax.rem(row * tile_rows, cols)
    inv = 1.0 / jnp.maximum(cnt_scr[pl.ds(pl.multiple_of(start, 8), tile_rows), :], 1.0)
    zero = jnp.zeros((seqs, LANES), F32)
    ops = []
    for d2 in range(pack):
        for q in range(groups):
            rows = []
            for v in lefts:
                rows += [v[q * seqs : (q + 1) * seqs] if k == d2 else zero for k in range(pack)]
            ops.append(jnp.concatenate(rows, 0).T.astype(BF16))
    a_ext = jnp.concatenate(ops, 0)

    for t in range(0, tiles, 2):
        rhs = jnp.concatenate(
            [jnp.concatenate([right(b, u) for b in range(blocks)], 0) for u in (t, t + 1)], 1
        )
        out = dot(a_ext, rhs)
        for k in range(2):
            for d2 in range(pack):
                for i in range(tile_rows):
                    at = (d2 * tile_rows + i) * chans
                    val = out[at : at + chans, k * cols : (k + 1) * cols] * inv[i : i + 1]
                    d = (t + k) * pack + d2
                    o_scr[i, d * chans : (d + 1) * chans, :] = val.astype(BF16)

    w_o = wo_ref[...]
    w_p = wp_ref[...]
    live_j = pres_ref[pl.ds(col, 1), :].astype(F32)
    live_i = pres_ref[pl.ds(lax.div(row * tile_rows, cols), 1), :].astype(F32)
    cnt_scr[0:LANES, :] = jnp.broadcast_to(live_i, (LANES, cols)).T
    live_rows = cnt_scr[pl.ds(pl.multiple_of(start, 8), tile_rows), :]
    for i in range(0, tile_rows, 2):
        upd = dot(w_o, jnp.concatenate([o_scr[i], o_scr[i + 1]], 1))
        normed = []
        for k in range(2):
            first = contact_ref[i + k] + upd[:, k * cols : (k + 1) * cols]
            first_ref[i + k] = first
            centred = first - jnp.mean(first, 0, keepdims=True)
            spread = jnp.mean(centred * centred, 0, keepdims=True)
            normed.append((centred * lax.rsqrt(spread + EPS)).astype(BF16))
        raw = dot(w_p, jnp.concatenate(normed, 1))
        for k in range(2):
            live = live_rows[i + k : i + k + 1] * live_j
            part = raw[:, k * cols : (k + 1) * cols]
            for side in range(2):
                at = side * 2 * width
                val = part[at : at + width] * sigmoid(part[at + width : at + 2 * width]) * live
                pan_scr[side, pl.ds(i + k, width, stride=tile_rows), :] = val
            gate_ref[i + k] = sigmoid(part[4 * width : 4 * width + feats])
    for ch in range(width):
        for side in range(2):
            panel_ref[ch, side] = pan_scr[side, ch * tile_rows : (ch + 1) * tile_rows, :].astype(BF16)


def triangle_kernel(recv_ref, out_ref, *, n_rows, n_cols):
    own = recv_ref.shape[1]
    tile_rows, cols = recv_ref.shape[3:]
    for ch in range(own):
        sides = [
            jnp.concatenate(
                [
                    jnp.concatenate([recv_ref[r * n_cols + x, ch, side] for r in range(n_rows)], 0)
                    for x in range(n_cols)
                ],
                1,
            )
            for side in range(2)
        ]
        prod = dot_nt(sides[0], sides[1]).astype(BF16)
        for r in range(n_rows):
            for x in range(n_cols):
                out_ref[r * n_cols + x, ch] = prod[
                    r * tile_rows : (r + 1) * tile_rows, x * cols : (x + 1) * cols
                ]


def finish_kernel(prod_ref, first_ref, gate_ref, we_ref, w1_ref, w2_ref, out_ref, mix):
    chans, tile_rows, cols = prod_ref.shape
    total = jnp.zeros((tile_rows, cols), F32)
    for ch in range(chans):
        total = total + prod_ref[ch].astype(F32)
    mean = total * (1.0 / chans)
    square = jnp.zeros((tile_rows, cols), F32)
    for ch in range(chans):
        centred = prod_ref[ch].astype(F32) - mean
        square = square + centred * centred
    scale = lax.rsqrt(square * (1.0 / chans) + EPS)
    for ch in range(chans):
        mix[ch * tile_rows : (ch + 1) * tile_rows, :] = (prod_ref[ch].astype(F32) - mean) * scale
    w_e, w_1, w_2 = we_ref[...], w1_ref[...], w2_ref[...]
    for i in range(0, tile_rows, 2):
        mixed = jnp.concatenate(
            [mix[pl.ds(i + k, chans, stride=tile_rows), :].astype(BF16) for k in range(2)], 1
        )
        proj = dot(w_e, mixed)
        seconds, normed = [], []
        for k in range(2):
            second = first_ref[i + k] + gate_ref[i + k] * proj[:, k * cols : (k + 1) * cols]
            centred = second - jnp.mean(second, 0, keepdims=True)
            spread = jnp.mean(centred * centred, 0, keepdims=True)
            seconds.append(second)
            normed.append((centred * lax.rsqrt(spread + EPS)).astype(BF16))
        hidden = jnp.maximum(dot(w_1, jnp.concatenate(normed, 1)), 0.0).astype(BF16)
        out = dot(w_2, hidden)
        for k in range(2):
            out_ref[i + k] = (seconds[k] + out[:, k * cols : (k + 1) * cols]).T


def on_device(
    family_representation,
    family_keep_flags,
    amino_presence,
    contact_embedding,
    couple_lhs_weights,
    couple_rhs_weights,
    pairwise_final_matrix,
    edge_source_matrix,
    edge_target_matrix,
    edge_final_sigmoid_matrix,
    edge_final_matrix,
    feedforward_expand_matrix,
    feedforward_shrink_matrix,
):
    seqs, cols, feats = family_representation.shape
    tile_rows, _, pair_feats = contact_embedding.shape
    n_rows = lax.axis_size("rows")
    n_cols = lax.axis_size("cols")
    chans = couple_lhs_weights.shape[1]
    width = edge_source_matrix.shape[1] // 2
    devices = n_rows * n_cols
    radix = n_rows // 4
    pieces = cols // tile_rows
    col = lax.axis_index("cols")
    presence = amino_presence.reshape(n_cols, cols)
    shape = jax.ShapeDtypeStruct

    right_rows = chans * seqs + TILE
    left_rows = tile_rows * chans * seqs // LANES + TILE
    right, left = call(
        functools.partial(project_kernel, tile_rows=tile_rows),
        (shape((right_rows, cols), BF16), shape((pieces, left_rows, LANES), BF16)),
        [pltpu.VMEM((feats // LANES, seqs * cols, LANES), F32), pltpu.VMEM((chans * seqs, cols), F32)],
        "project",
    )(family_representation, family_keep_flags, presence, couple_lhs_weights.T, couple_rhs_weights.T)

    row = lax.axis_index("rows")
    left_wide = jnp.zeros((n_cols, pieces, left_rows, LANES), BF16)
    left_wide = lax.dynamic_update_slice_in_dim(left_wide, left[None], col, 0)
    for k in range(1, n_cols):
        got = lax.ppermute(left, "cols", [(i, (i + k) % n_cols) for i in range(n_cols)])
        left_wide = lax.dynamic_update_slice_in_dim(left_wide, got[None], (col + n_cols - k) % n_cols, 0)
    left_wide = left_wide.reshape(radix, 2, 2, left_rows, LANES)

    def shift(k):
        return [(i, (i + 4 * k) % n_rows) for i in range(n_rows)]

    right_z = jnp.stack([right] + [lax.ppermute(right, "rows", shift(k)) for k in range(1, radix)])
    pair_y = [(i, i ^ 2) for i in range(n_rows)]
    pair_c = [(i, i ^ 1) for i in range(n_rows)]
    right_y = lax.ppermute(right_z, "rows", pair_y)

    def pick(array, index, axis):
        return lax.dynamic_index_in_dim(array, index, axis, keepdims=False)

    left_z = [pick(left_wide, row // 4, 0)]
    for k in range(1, radix):
        left_z.append(lax.ppermute(pick(left_wide, (row // 4 + k) % radix, 0), "rows", shift(k)))
    left_z = jnp.stack(left_z)
    right0 = jnp.concatenate([right_z, right_y], 0)
    right1 = lax.ppermute(right0, "rows", pair_c)
    y, c = (row // 2) % 2, row % 2
    left_y = jnp.stack([pick(left_z, y, 1), lax.ppermute(pick(left_z, 1 - y, 1), "rows", pair_y)])
    left_y = left_y.reshape(2 * radix, 2, left_rows, LANES)
    left0 = pick(left_y, c, 1)
    left1 = lax.ppermute(pick(left_y, 1 - c, 1), "rows", pair_c)

    contact_t = contact_embedding.transpose(0, 2, 1)
    w_o = pairwise_final_matrix.reshape(chans, chans, pair_feats).transpose(2, 1, 0).reshape(pair_feats, chans * chans)
    w_p = jnp.concatenate([edge_source_matrix, edge_target_matrix, edge_final_sigmoid_matrix], 1).T
    pair = shape((tile_rows, pair_feats, cols), F32)
    first, gate, panels = call(
        functools.partial(pair_kernel, seqs=seqs, tile_rows=tile_rows, chans=chans),
        (pair, pair, shape((width, 2, tile_rows, cols), BF16)),
        [
            pltpu.VMEM((tile_rows, chans * chans, cols), BF16),
            pltpu.VMEM((LANES, cols), F32),
            pltpu.VMEM((2, width * tile_rows, cols), F32),
        ],
        "pair",
    )(right0, right1, left0, left1, contact_t, presence, w_o, w_p)

    panels = lax.all_to_all(
        panels.reshape(devices, width // devices, 2, tile_rows, cols),
        ("rows", "cols"), split_axis=0, concat_axis=0, tiled=True,
    )
    product = call(
        functools.partial(triangle_kernel, n_rows=n_rows, n_cols=n_cols),
        shape((devices, width // devices, tile_rows, cols), BF16),
        [],
        "triangle",
    )(panels)
    product = lax.all_to_all(product, ("rows", "cols"), split_axis=0, concat_axis=0, tiled=True)
    return call(
        finish_kernel,
        shape((tile_rows, cols, pair_feats), F32),
        [pltpu.VMEM((width * tile_rows, cols), F32)],
        "finish",
    )(
        product.reshape(width, tile_rows, cols), first, gate,
        edge_final_matrix.T, feedforward_expand_matrix.T, feedforward_shrink_matrix.T,
    )


def solution(mesh):
    tiles = P(("crops", "rows"), "cols", None)
    in_specs = (tiles, P(("crops", "rows"), "cols"), P("crops"), tiles) + (P(),) * 9
    return jax.shard_map(on_device, mesh=mesh, in_specs=in_specs, out_specs=tiles, check_vma=False)
```

```python
import functools

import jax
import jax.numpy as jnp
from jax import lax
from jax.experimental import pallas as pl
from jax.experimental.pallas import tpu as pltpu
from jax.sharding import PartitionSpec as P

EPS = 1e-05
F32 = jnp.float32
BF16 = jnp.bfloat16
TILE = 16
LANES = 128
VMEM_LIMIT = 32 * 2**20
VMEM = pl.BlockSpec(memory_space=pltpu.VMEM)


def dot(a, b):
    return lax.dot_general(a, b, (((1,), (0,)), ((), ())), preferred_element_type=F32)


def dot_nt(a, b):
    return lax.dot_general(a, b, (((1,), (1,)), ((), ())), preferred_element_type=F32)


def sigmoid(x):
    return 0.5 * jnp.tanh(0.5 * x) + 0.5


def call(kernel, out_shape, scratch, name, ins=(), out_specs=None):
    def run(*args):
        args = [
            pltpu.with_memory_space_constraint(x, pltpu.VMEM) if k in ins else x for k, x in enumerate(args)
        ]
        return pl.pallas_call(
            kernel,
            out_shape=out_shape,
            in_specs=[VMEM] * len(args),
            out_specs=out_specs or jax.tree.map(lambda _: VMEM, out_shape),
            scratch_shapes=scratch,
            compiler_params=pltpu.CompilerParams(vmem_limit_bytes=VMEM_LIMIT),
            name=name,
        )(*args)

    return run


def project_kernel(fam_ref, keep_ref, pres_ref, wl_ref, wr_ref, right_ref, left_ref, nf, rs, *, tile_rows):
    seqs, cols, feats = fam_ref.shape
    chans = wl_ref.shape[0]
    col = lax.axis_index("cols")
    live = (keep_ref[...] * pres_ref[pl.ds(col, 1), :]).astype(F32)
    live_t = jnp.concatenate([live, jnp.zeros((LANES - seqs, cols), F32)], 0).T
    wr_t = wr_ref[...]
    for s in range(seqs):
        v = fam_ref[s]
        centred = v - jnp.mean(v, -1, keepdims=True)
        spread = jnp.mean(centred * centred, -1, keepdims=True)
        n = centred * (lax.rsqrt(spread + EPS) * live_t[:, s : s + 1])
        for h in range(feats // LANES):
            nf[h, pl.ds(s * cols, cols), :] = n[:, h * LANES : (h + 1) * LANES]
        rs[pl.ds(s, chans, stride=seqs), :] = dot_nt(wr_t, n.astype(BF16))
    right_ref[0 : chans * seqs, :] = rs[...].astype(BF16)
    live_tile = jnp.concatenate([live, jnp.zeros((TILE - seqs, cols), F32)], 0).astype(BF16)
    right_ref[chans * seqs : chans * seqs + TILE, :] = live_tile
    per = LANES // chans
    groups = tile_rows // per
    pieces = cols // tile_rows
    wl = wl_ref[...].astype(F32).T
    acc = None
    for i4 in range(per):
        parts = []
        if i4:
            parts.append(jnp.zeros((feats, i4 * chans), F32))
        parts.append(wl)
        if i4 < per - 1:
            parts.append(jnp.zeros((feats, (per - 1 - i4) * chans), F32))
        w = jnp.concatenate(parts, 1).astype(BF16)
        rows = [
            jnp.concatenate(
                [nf[h, pl.ds(pq * per + i4, seqs, stride=cols), :] for h in range(feats // LANES)], 1
            )
            for pq in range(pieces * groups)
        ]
        part = dot(jnp.concatenate(rows, 0).astype(BF16), w)
        acc = part if acc is None else acc + part
    block = groups * seqs
    planes = left_ref.shape[0]
    row = lax.axis_index("rows")
    z, y, c = lax.div(row, 4), lax.rem(lax.div(row, 2), 2), lax.rem(row, 2)
    for p in range(pieces):
        at = (
            lax.rem(p // 4 + planes - lax.rem(z, planes), planes),
            lax.rem((p // 2) % 2 + y, 2),
            lax.rem(p % 2 + c, 2),
        )
        left_ref[at[0], at[1], at[2], 0:block, :] = acc[p * block : (p + 1) * block].astype(BF16)
        left_ref[at[0], at[1], at[2], block : block + TILE, :] = live_tile


def prepare_kernel(contact_ref, wo_ref, src_ref, tgt_ref, gate_ref, after_ref, contact_t_ref, wo_t_ref, wp_t_ref, scr):
    tile_rows = contact_ref.shape[0]
    rows = wo_ref.shape[0]
    chans = int(rows**0.5)
    for i in range(tile_rows):
        contact_t_ref[i] = contact_ref[i].T
    scr[...] = wo_ref[...].astype(F32)
    for at in range(0, rows, LANES):
        part = jnp.concatenate(
            [scr[pl.ds(d, chans, stride=chans), :] for d in range(at // chans, (at + LANES) // chans)], 0
        )
        wo_t_ref[:, at : at + LANES] = part.T.astype(BF16)
    at = 0
    for ref in (src_ref, tgt_ref, gate_ref):
        wp_t_ref[at : at + ref.shape[1], :] = ref[...].astype(F32).T.astype(BF16)
        at += ref.shape[1]


def pair_kernel(*refs, seqs, radix, tile_rows, chans):
    z_refs, refs = refs[:radix], refs[radix:]
    (y_ref, c_ref, left_ref, contact_ref, pres_ref, wo_ref, wp_ref,
     first_ref, gate_ref, panel_ref, o_scr, cnt_scr, pan_scr) = refs
    right_rows, cols = z_refs[0].shape
    left_rows = left_ref.shape[3]
    tiles = right_rows // TILE - 1
    blocks = 4 * radix
    feats = first_ref.shape[1]
    width = pan_scr.shape[1] // tile_rows
    pack = TILE // seqs
    per = LANES // chans
    groups = tile_rows // per
    row = lax.axis_index("rows")
    col = lax.axis_index("cols")
    z = lax.div(row, 4)
    planes = cols // tile_rows // 4
    turn = col * planes + lax.rem(z, planes) - z + radix

    def right(b, t):
        core, pair, k = b // (2 * radix), b // radix % 2, b % radix
        if core:
            ref, at = c_ref, (pair * radix + k) * right_rows
        elif pair:
            ref, at = y_ref, k * right_rows
        else:
            ref, at = z_refs[k], 0
        return ref[at + t * TILE : at + (t + 1) * TILE, :]

    def left(b):
        core, pair, k = b // (2 * radix), b // radix % 2, b % radix
        m = lax.rem(turn + k, radix)
        if not core and not pair:
            return left_ref[m, 0, 0]
        if core:
            ref, at = c_ref, 2 * radix * right_rows + (pair * radix + m) * left_rows
        else:
            ref, at = y_ref, radix * right_rows + 2 * m * left_rows
        return ref[pl.ds(pl.multiple_of(at, TILE), left_rows), :]

    lefts = [left(b).astype(F32) for b in range(blocks)]
    block = groups * seqs
    live_l = jnp.concatenate([v[block : block + seqs] for v in lefts], 0).T.astype(BF16)
    live_r = jnp.concatenate([right(b, tiles).astype(F32)[:seqs] for b in range(blocks)], 0).astype(BF16)
    cnt_scr[...] = dot(live_l, live_r)
    start = lax.rem(row * tile_rows, cols)
    inv = 1.0 / jnp.maximum(cnt_scr[pl.ds(pl.multiple_of(start, 8), tile_rows), :], 1.0)
    zero = jnp.zeros((seqs, LANES), F32)
    ops = []
    for d2 in range(pack):
        for q in range(groups):
            rows = []
            for v in lefts:
                rows += [v[q * seqs : (q + 1) * seqs] if k == d2 else zero for k in range(pack)]
            ops.append(jnp.concatenate(rows, 0).T.astype(BF16))
    a_ext = jnp.concatenate(ops, 0)

    for t in range(0, tiles, 2):
        rhs = jnp.concatenate(
            [jnp.concatenate([right(b, u) for b in range(blocks)], 0) for u in (t, t + 1)], 1
        )
        out = dot(a_ext, rhs)
        for k in range(2):
            for d2 in range(pack):
                for i in range(tile_rows):
                    at = (d2 * tile_rows + i) * chans
                    val = out[at : at + chans, k * cols : (k + 1) * cols] * inv[i : i + 1]
                    d = (t + k) * pack + d2
                    o_scr[i, d * chans : (d + 1) * chans, :] = val.astype(BF16)

    w_o = wo_ref[...]
    w_p = wp_ref[...]
    live_j = pres_ref[pl.ds(col, 1), :].astype(F32)
    live_i = pres_ref[pl.ds(lax.div(row * tile_rows, cols), 1), :].astype(F32)
    cnt_scr[0:LANES, :] = jnp.broadcast_to(live_i, (LANES, cols)).T
    live_rows = cnt_scr[pl.ds(pl.multiple_of(start, 8), tile_rows), :]
    for i in range(0, tile_rows, 2):
        upd = dot(w_o, jnp.concatenate([o_scr[i], o_scr[i + 1]], 1))
        normed = []
        for k in range(2):
            first = contact_ref[i + k] + upd[:, k * cols : (k + 1) * cols]
            first_ref[i + k] = first
            centred = first - jnp.mean(first, 0, keepdims=True)
            spread = jnp.mean(centred * centred, 0, keepdims=True)
            normed.append((centred * lax.rsqrt(spread + EPS)).astype(BF16))
        raw = dot(w_p, jnp.concatenate(normed, 1))
        for k in range(2):
            live = live_rows[i + k : i + k + 1] * live_j
            part = raw[:, k * cols : (k + 1) * cols]
            for side in range(2):
                at = side * 2 * width
                val = part[at : at + width] * sigmoid(part[at + width : at + 2 * width]) * live
                pan_scr[side, pl.ds(i + k, width, stride=tile_rows), :] = val
            gate_ref[i + k] = sigmoid(part[4 * width : 4 * width + feats])
    for ch in range(width):
        for side in range(2):
            panel_ref[ch, side] = pan_scr[side, ch * tile_rows : (ch + 1) * tile_rows, :].astype(BF16)


def triangle_kernel(recv_ref, out_ref, *, n_rows, n_cols):
    own = recv_ref.shape[1]
    tile_rows, cols = recv_ref.shape[3:]
    for ch in range(own):
        sides = [
            jnp.concatenate(
                [
                    jnp.concatenate([recv_ref[r * n_cols + x, ch, side] for r in range(n_rows)], 0)
                    for x in range(n_cols)
                ],
                1,
            )
            for side in range(2)
        ]
        prod = dot_nt(sides[0], sides[1]).astype(BF16)
        for r in range(n_rows):
            for x in range(n_cols):
                out_ref[r * n_cols + x, ch] = prod[
                    r * tile_rows : (r + 1) * tile_rows, x * cols : (x + 1) * cols
                ]


def finish_kernel(prod_ref, first_ref, gate_ref, we_ref, w1_ref, w2_ref, hbm_ref, mix, out_ref, sems):
    chans, tile_rows, cols = prod_ref.shape
    total = jnp.zeros((tile_rows, cols), F32)
    for ch in range(chans):
        total = total + prod_ref[ch].astype(F32)
    mean = total * (1.0 / chans)
    square = jnp.zeros((tile_rows, cols), F32)
    for ch in range(chans):
        centred = prod_ref[ch].astype(F32) - mean
        square = square + centred * centred
    scale = lax.rsqrt(square * (1.0 / chans) + EPS)
    for ch in range(chans):
        mix[ch * tile_rows : (ch + 1) * tile_rows, :] = (prod_ref[ch].astype(F32) - mean) * scale
    w_e, w_1, w_2 = we_ref[...], w1_ref[...], w2_ref[...]
    copies = []
    for i in range(0, tile_rows, 2):
        mixed = jnp.concatenate(
            [mix[pl.ds(i + k, chans, stride=tile_rows), :].astype(BF16) for k in range(2)], 1
        )
        proj = dot(w_e, mixed)
        seconds, normed = [], []
        for k in range(2):
            second = first_ref[i + k] + gate_ref[i + k] * proj[:, k * cols : (k + 1) * cols]
            centred = second - jnp.mean(second, 0, keepdims=True)
            spread = jnp.mean(centred * centred, 0, keepdims=True)
            seconds.append(second)
            normed.append((centred * lax.rsqrt(spread + EPS)).astype(BF16))
        hidden = jnp.maximum(dot(w_1, jnp.concatenate(normed, 1)), 0.0).astype(BF16)
        out = dot(w_2, hidden)
        for k in range(2):
            out_ref[i + k] = (seconds[k] + out[:, k * cols : (k + 1) * cols]).T
        copy = pltpu.make_async_copy(out_ref.at[pl.ds(i, 2)], hbm_ref.at[pl.ds(i, 2)], sems.at[i // 2])
        copy.start()
        copies.append(copy)
    for copy in copies:
        copy.wait()


def on_device(
    family_representation,
    family_keep_flags,
    amino_presence,
    contact_embedding,
    couple_lhs_weights,
    couple_rhs_weights,
    pairwise_final_matrix,
    edge_source_matrix,
    edge_target_matrix,
    edge_final_sigmoid_matrix,
    edge_final_matrix,
    feedforward_expand_matrix,
    feedforward_shrink_matrix,
):
    seqs, cols, feats = family_representation.shape
    tile_rows, _, pair_feats = contact_embedding.shape
    n_rows = lax.axis_size("rows")
    n_cols = lax.axis_size("cols")
    chans = couple_lhs_weights.shape[1]
    width = edge_source_matrix.shape[1] // 2
    devices = n_rows * n_cols
    radix = n_rows // 4
    pieces = cols // tile_rows
    col = lax.axis_index("cols")
    presence = amino_presence.reshape(n_cols, cols)
    shape = pltpu.VMEM
    planes = pieces // 4

    right_rows = chans * seqs + TILE
    left_rows = tile_rows * chans * seqs // LANES + TILE
    right, left = call(
        functools.partial(project_kernel, tile_rows=tile_rows),
        (shape((right_rows, cols), BF16), shape((planes, 2, 2, left_rows, LANES), BF16)),
        [pltpu.VMEM((feats // LANES, seqs * cols, LANES), F32), pltpu.VMEM((chans * seqs, cols), F32)],
        "project",
    )(family_representation, family_keep_flags, presence, couple_lhs_weights.T, couple_rhs_weights.T)

    zs = [right]
    for k in range(1, radix):
        zs.append(lax.ppermute(right, "rows", [(i, (i + 4 * k) % n_rows) for i in range(n_rows)]))
    lefts = []
    for m in range(radix):
        perm = []
        for i in range(n_rows):
            for x in range(n_cols):
                to = (i // 4 + m) % radix
                target = (x * planes + to % planes) * 4 + i % 4
                perm.append((i * n_cols + x, target * n_cols + to // planes))
        lefts.append(lax.ppermute(left[m % planes], ("rows", "cols"), perm))
    lefts = jnp.stack(lefts)

    def rows_of(array):
        return array.reshape(-1, LANES)

    y_msg = jnp.concatenate(zs + [rows_of(lefts[:, 1])], 0)
    y_got = lax.ppermute(y_msg, "rows", [(i, i ^ 2) for i in range(n_rows)])
    cut = radix * right_rows
    c_msg = jnp.concatenate(
        zs + [
            y_got[:cut],
            rows_of(lefts[:, 0, 1]),
            rows_of(y_got[cut:].reshape(radix, 2, left_rows, LANES)[:, 1]),
        ], 0
    )
    c_got = lax.ppermute(c_msg, "rows", [(i, i ^ 1) for i in range(n_rows)])

    pair = shape((tile_rows, pair_feats, cols), F32)
    contact_t, w_o, w_p = call(
        prepare_kernel,
        (pair, shape((pair_feats, chans * chans), BF16), shape((4 * width + pair_feats, pair_feats), BF16)),
        [pltpu.VMEM((chans * chans, pair_feats), F32)],
        "prepare",
        ins=(5,),
    )(
        contact_embedding, pairwise_final_matrix, edge_source_matrix, edge_target_matrix,
        edge_final_sigmoid_matrix, zs[-1],
    )
    args = zs + [y_got, c_got, lefts, contact_t, presence, w_o, w_p]
    first, gate, panels = call(
        functools.partial(pair_kernel, seqs=seqs, radix=radix, tile_rows=tile_rows, chans=chans),
        (pair, pair, shape((width, 2, tile_rows, cols), BF16)),
        [
            pltpu.VMEM((tile_rows, chans * chans, cols), BF16),
            pltpu.VMEM((LANES, cols), F32),
            pltpu.VMEM((2, width * tile_rows, cols), F32),
        ],
        "pair",
        ins=[k for k in range(len(args)) if k != len(args) - 3],
    )(*args)

    panels = lax.all_to_all(
        panels.reshape(devices, width // devices, 2, tile_rows, cols),
        ("rows", "cols"), split_axis=0, concat_axis=0, tiled=True,
    )
    product = call(
        functools.partial(triangle_kernel, n_rows=n_rows, n_cols=n_cols),
        shape((devices, width // devices, tile_rows, cols), BF16),
        [],
        "triangle",
        ins=(0,),
    )(panels)
    product = lax.all_to_all(product, ("rows", "cols"), split_axis=0, concat_axis=0, tiled=True)
    return call(
        finish_kernel,
        jax.ShapeDtypeStruct((tile_rows, cols, pair_feats), F32),
        [
            pltpu.VMEM((width * tile_rows, cols), F32),
            pltpu.VMEM((tile_rows, cols, pair_feats), F32),
            pltpu.SemaphoreType.DMA((tile_rows // 2,)),
        ],
        "finish",
        ins=(0, 1, 2, 3, 4, 5),
        out_specs=pl.BlockSpec(memory_space=pl.ANY),
    )(
        product.reshape(width, tile_rows, cols), first, gate,
        edge_final_matrix.T, feedforward_expand_matrix.T, feedforward_shrink_matrix.T,
    )


def solution(mesh):
    tiles = P(("crops", "rows"), "cols", None)
    in_specs = (tiles, P(("crops", "rows"), "cols"), P("crops"), tiles) + (P(),) * 9
    return jax.shard_map(on_device, mesh=mesh, in_specs=in_specs, out_specs=tiles, check_vma=False)
```

```python
import functools

import jax
import jax.numpy as jnp
from jax import lax
from jax.experimental import pallas as pl
from jax.experimental.pallas import tpu as pltpu
from jax.sharding import PartitionSpec as P


EPS = 1e-05
F32 = jnp.float32
BF16 = jnp.bfloat16
TILE = 16
LANES = 128
VMEM_LIMIT = 32 * 2**20
VMEM = pl.BlockSpec(memory_space=pltpu.VMEM)


def dot(a, b):
    return lax.dot_general(a, b, (((1,), (0,)), ((), ())), preferred_element_type=F32)


def dot_nt(a, b):
    return lax.dot_general(a, b, (((1,), (1,)), ((), ())), preferred_element_type=F32)


def sigmoid(x):
    return 0.5 * jnp.tanh(0.5 * x) + 0.5


def call(kernel, out_shape, scratch, ins=(), hbm=(), out_specs=None):
    def run(*args):
        args = [
            pltpu.with_memory_space_constraint(x, pltpu.VMEM if k in ins else pltpu.HBM)
            if k in ins or k in hbm
            else x
            for k, x in enumerate(args)
        ]
        return pl.pallas_call(
            kernel,
            out_shape=out_shape,
            in_specs=[VMEM] * len(args),
            out_specs=out_specs or jax.tree.map(lambda _: VMEM, out_shape),
            scratch_shapes=scratch,
            compiler_params=pltpu.CompilerParams(vmem_limit_bytes=VMEM_LIMIT),
        )(*args)

    return run


def project_kernel(fam_ref, keep_ref, pres_ref, wl_ref, wr_ref, right_ref, left_ref, nf, rs, *, tile_rows):
    seqs, cols, feats = fam_ref.shape
    chans = wl_ref.shape[0]
    col = lax.axis_index("cols")
    live = (keep_ref[...] * pres_ref[pl.ds(col, 1), :]).astype(F32)
    live_t = jnp.concatenate([live, jnp.zeros((LANES - seqs, cols), F32)], 0).T
    wr_t = wr_ref[...]
    for s in range(seqs):
        v = fam_ref[s]
        centred = v - jnp.mean(v, -1, keepdims=True)
        spread = jnp.mean(centred * centred, -1, keepdims=True)
        n = centred * (lax.rsqrt(spread + EPS) * live_t[:, s : s + 1])
        for h in range(feats // LANES):
            nf[h, pl.ds(s * cols, cols), :] = n[:, h * LANES : (h + 1) * LANES]
        rs[pl.ds(s, chans, stride=seqs), :] = dot_nt(wr_t, n.astype(BF16))
    right_ref[0 : chans * seqs, :] = rs[...].astype(BF16)
    live_tile = jnp.concatenate([live, jnp.zeros((TILE - seqs, cols), F32)], 0).astype(BF16)
    right_ref[chans * seqs : chans * seqs + TILE, :] = live_tile
    per = LANES // chans
    groups = tile_rows // per
    pieces = cols // tile_rows
    wl = wl_ref[...].astype(F32).T
    acc = None
    for i4 in range(per):
        parts = []
        if i4:
            parts.append(jnp.zeros((feats, i4 * chans), F32))
        parts.append(wl)
        if i4 < per - 1:
            parts.append(jnp.zeros((feats, (per - 1 - i4) * chans), F32))
        w = jnp.concatenate(parts, 1).astype(BF16)
        rows = [
            jnp.concatenate(
                [nf[h, pl.ds(pq * per + i4, seqs, stride=cols), :] for h in range(feats // LANES)], 1
            )
            for pq in range(pieces * groups)
        ]
        part = dot(jnp.concatenate(rows, 0).astype(BF16), w)
        acc = part if acc is None else acc + part
    block = groups * seqs
    row = lax.axis_index("rows")
    y, c = lax.rem(lax.div(row, 2), 2), lax.rem(row, 2)
    for p in range(pieces):
        at = (p // 4, lax.rem((p // 2) % 2 + y, 2), lax.rem(p % 2 + c, 2))
        left_ref[at[0], at[1], at[2], 0:block, :] = acc[p * block : (p + 1) * block].astype(BF16)
        left_ref[at[0], at[1], at[2], block : block + TILE, :] = live_tile


def prepare_kernel(
    contact_ref, wo_ref, src_ref, tgt_ref, gate_ref, pres_ref, after_ref,
    contact_t_ref, wo_t_ref, wp_t_ref, live_ref,
    scr, column,
):
    tile_rows = contact_ref.shape[0]
    rows = wo_ref.shape[0]
    chans = int(rows**0.5)
    for i in range(tile_rows):
        contact_t_ref[i] = contact_ref[i].T
    scr[...] = wo_ref[...].astype(F32)
    for at in range(0, rows, LANES):
        part = jnp.concatenate(
            [scr[pl.ds(d, chans, stride=chans), :] for d in range(at // chans, (at + LANES) // chans)], 0
        )
        wo_t_ref[:, at : at + LANES] = part.T.astype(BF16)
    at = 0
    for ref in (src_ref, tgt_ref, gate_ref):
        wp_t_ref[at : at + ref.shape[1], :] = ref[...].astype(F32).T.astype(BF16)
        at += ref.shape[1]
    cols = contact_ref.shape[1]
    start = lax.axis_index("rows") * tile_rows
    live_i = pres_ref[pl.ds(lax.div(start, cols), 1), :].astype(F32)
    column[...] = jnp.broadcast_to(live_i, (LANES, cols)).T
    live_j = pres_ref[pl.ds(lax.axis_index("cols"), 1), :].astype(F32)
    live_ref[...] = column[pl.ds(pl.multiple_of(lax.rem(start, cols), 8), tile_rows), :] * live_j


def pair_kernel(
    z_ref, y_ref, c_ref, left_z_ref, left_y_ref, left_c_ref, contact_ref, live_ref, wo_ref, wp_ref,
    first_ref, gate_ref, panel_ref,
    o_scr, cnt_scr, pan_scr,
    *, seqs, radix, tile_rows, chans,
):
    right_rows, cols = z_ref.shape[0] // radix, z_ref.shape[1]
    tiles = right_rows // TILE - 1
    blocks = 4 * radix
    feats = first_ref.shape[1]
    width = pan_scr.shape[1] // tile_rows
    pack = TILE // seqs
    per = LANES // chans
    groups = tile_rows // per
    row = lax.axis_index("rows")

    def right(b, t):
        core, pair, k = b // (2 * radix), b // radix % 2, b % radix
        ref, at = (c_ref, pair * radix + k) if core else (y_ref if pair else z_ref, k)
        return ref[at * right_rows + t * TILE : at * right_rows + (t + 1) * TILE, :]

    def left(b):
        core, pair, k = b // (2 * radix), b // radix % 2, b % radix
        if core:
            return left_c_ref[pair * radix + k]
        return left_y_ref[k, 0] if pair else left_z_ref[k, 0, 0]

    lefts = [left(b).astype(F32) for b in range(blocks)]
    block = groups * seqs
    live_l = jnp.concatenate([v[block : block + seqs] for v in lefts], 0).T.astype(BF16)
    live_r = jnp.concatenate([right(b, tiles).astype(F32)[:seqs] for b in range(blocks)], 0).astype(BF16)
    cnt_scr[...] = dot(live_l, live_r)
    start = lax.rem(row * tile_rows, cols)
    inv = 1.0 / jnp.maximum(cnt_scr[pl.ds(pl.multiple_of(start, 8), tile_rows), :], 1.0)
    zero = jnp.zeros((seqs, LANES), F32)
    ops = []
    for d2 in range(pack):
        for q in range(groups):
            rows = []
            for v in lefts:
                rows += [v[q * seqs : (q + 1) * seqs] if k == d2 else zero for k in range(pack)]
            ops.append(jnp.concatenate(rows, 0).T.astype(BF16))
    a_ext = jnp.concatenate(ops, 0)

    for t in range(0, tiles, 2):
        rhs = jnp.concatenate(
            [jnp.concatenate([right(b, u) for b in range(blocks)], 0) for u in (t, t + 1)], 1
        )
        out = dot(a_ext, rhs)
        for k in range(2):
            for d2 in range(pack):
                for i in range(tile_rows):
                    at = (d2 * tile_rows + i) * chans
                    val = out[at : at + chans, k * cols : (k + 1) * cols] * inv[i : i + 1]
                    d = (t + k) * pack + d2
                    o_scr[i, d * chans : (d + 1) * chans, :] = val.astype(BF16)

    w_o = wo_ref[...]
    w_p = wp_ref[...]
    for i in range(0, tile_rows, 2):
        upd = dot(w_o, jnp.concatenate([o_scr[i], o_scr[i + 1]], 1))
        normed = []
        for k in range(2):
            first = contact_ref[i + k] + upd[:, k * cols : (k + 1) * cols]
            first_ref[i + k] = first
            centred = first - jnp.mean(first, 0, keepdims=True)
            spread = jnp.mean(centred * centred, 0, keepdims=True)
            normed.append((centred * lax.rsqrt(spread + EPS)).astype(BF16))
        raw = dot(w_p, jnp.concatenate(normed, 1))
        for k in range(2):
            live = live_ref[i + k : i + k + 1, :]
            part = raw[:, k * cols : (k + 1) * cols]
            for side in range(2):
                at = side * 2 * width
                val = part[at : at + width] * sigmoid(part[at + width : at + 2 * width]) * live
                pan_scr[side, pl.ds(i + k, width, stride=tile_rows), :] = val
            gate_ref[i + k] = sigmoid(part[4 * width : 4 * width + feats])
    for ch in range(width):
        for side in range(2):
            panel_ref[ch, side] = pan_scr[side, ch * tile_rows : (ch + 1) * tile_rows, :].astype(BF16)


def triangle_kernel(recv_ref, out_ref, *, n_rows, n_cols):
    own = recv_ref.shape[1]
    tile_rows, cols = recv_ref.shape[3:]
    for ch in range(own):
        sides = [
            jnp.concatenate(
                [
                    jnp.concatenate([recv_ref[r * n_cols + x, ch, side] for r in range(n_rows)], 0)
                    for x in range(n_cols)
                ],
                1,
            )
            for side in range(2)
        ]
        prod = dot_nt(sides[0], sides[1]).astype(BF16)
        for r in range(n_rows):
            for x in range(n_cols):
                out_ref[r * n_cols + x, ch] = prod[
                    r * tile_rows : (r + 1) * tile_rows, x * cols : (x + 1) * cols
                ]


def finish_kernel(prod_ref, first_ref, gate_ref, we_ref, w1_ref, w2_ref, hbm_ref, mix, out_ref, sems):
    chans, tile_rows, cols = prod_ref.shape
    total = jnp.zeros((tile_rows, cols), F32)
    for ch in range(chans):
        total = total + prod_ref[ch].astype(F32)
    mean = total * (1.0 / chans)
    square = jnp.zeros((tile_rows, cols), F32)
    for ch in range(chans):
        centred = prod_ref[ch].astype(F32) - mean
        square = square + centred * centred
    scale = lax.rsqrt(square * (1.0 / chans) + EPS)
    for ch in range(chans):
        mix[ch * tile_rows : (ch + 1) * tile_rows, :] = (prod_ref[ch].astype(F32) - mean) * scale
    w_e, w_1, w_2 = we_ref[...], w1_ref[...], w2_ref[...]
    copies = []
    for i in range(0, tile_rows, 2):
        mixed = jnp.concatenate(
            [mix[pl.ds(i + k, chans, stride=tile_rows), :].astype(BF16) for k in range(2)], 1
        )
        proj = dot(w_e, mixed)
        seconds, normed = [], []
        for k in range(2):
            second = first_ref[i + k] + gate_ref[i + k] * proj[:, k * cols : (k + 1) * cols]
            centred = second - jnp.mean(second, 0, keepdims=True)
            spread = jnp.mean(centred * centred, 0, keepdims=True)
            seconds.append(second)
            normed.append((centred * lax.rsqrt(spread + EPS)).astype(BF16))
        hidden = jnp.maximum(dot(w_1, jnp.concatenate(normed, 1)), 0.0).astype(BF16)
        out = dot(w_2, hidden)
        for k in range(2):
            out_ref[i + k] = (seconds[k] + out[:, k * cols : (k + 1) * cols]).T
        copy = pltpu.make_async_copy(out_ref.at[pl.ds(i, 2)], hbm_ref.at[pl.ds(i, 2)], sems.at[i // 2])
        copy.start()
        copies.append(copy)
    for copy in copies:
        copy.wait()


def on_device(
    family_representation,
    family_keep_flags,
    amino_presence,
    contact_embedding,
    couple_lhs_weights,
    couple_rhs_weights,
    pairwise_final_matrix,
    edge_source_matrix,
    edge_target_matrix,
    edge_final_sigmoid_matrix,
    edge_final_matrix,
    feedforward_expand_matrix,
    feedforward_shrink_matrix,
):
    seqs, cols, feats = family_representation.shape
    tile_rows, _, pair_feats = contact_embedding.shape
    n_rows = lax.axis_size("rows")
    n_cols = lax.axis_size("cols")
    chans = couple_lhs_weights.shape[1]
    width = edge_source_matrix.shape[1] // 2
    devices = n_rows * n_cols
    radix = n_rows // 4
    pieces = cols // tile_rows
    col = lax.axis_index("cols")
    presence = amino_presence.reshape(n_cols, cols)
    shape = pltpu.VMEM
    planes = pieces // 4

    right_rows = chans * seqs + TILE
    left_rows = tile_rows * chans * seqs // LANES + TILE
    right, left = call(
        functools.partial(project_kernel, tile_rows=tile_rows),
        (shape((right_rows, cols), BF16), shape((planes, 2, 2, left_rows, LANES), BF16)),
        [pltpu.VMEM((feats // LANES, seqs * cols, LANES), F32), pltpu.VMEM((chans * seqs, cols), F32)],
        hbm=(0, 1, 2, 3, 4),
    )(family_representation, family_keep_flags, presence, couple_lhs_weights.T, couple_rhs_weights.T)

    def shift(k):
        return [(i, (i + 4 * k) % n_rows) for i in range(n_rows)]

    pair_y = [(i, i ^ 2) for i in range(n_rows)]
    pair_c = [(i, i ^ 1) for i in range(n_rows)]
    zs = [right] + [lax.ppermute(right, "rows", shift(k)) for k in range(1, radix)]
    wide = jnp.zeros((n_cols,) + left.shape, BF16)
    wide = lax.dynamic_update_slice_in_dim(wide, left[None], col, 0)
    for k in range(1, n_cols):
        got = lax.ppermute(left, "cols", [(i, (i + k) % n_cols) for i in range(n_cols)])
        wide = lax.dynamic_update_slice_in_dim(wide, got[None], (col + n_cols - k) % n_cols, 0)
    wide = wide.reshape((radix,) + left.shape[1:])
    y_msg = jnp.concatenate(zs, 0)
    y_got = lax.ppermute(y_msg, "rows", pair_y)
    z = lax.axis_index("rows") // 4
    lefts = []
    for k in range(radix):
        piece = lax.dynamic_index_in_dim(wide, (z + k) % radix, 0, keepdims=False)
        lefts.append(lax.ppermute(piece, "rows", shift(k)) if k else piece)
    lefts = jnp.stack(lefts)
    c_got = lax.ppermute(jnp.concatenate([y_msg, y_got], 0), "rows", pair_c)
    left_y = lax.ppermute(lefts[:, 1], "rows", pair_y)
    left_c = lax.ppermute(jnp.concatenate([lefts[:, 0, 1], left_y[:, 1]], 0), "rows", pair_c)

    pair = shape((tile_rows, pair_feats, cols), F32)
    contact_t, w_o, w_p, live = call(
        prepare_kernel,
        (
            pair,
            shape((pair_feats, chans * chans), BF16),
            shape((4 * width + pair_feats, pair_feats), BF16),
            shape((tile_rows, cols), F32),
        ),
        [pltpu.VMEM((chans * chans, pair_feats), F32), pltpu.VMEM((cols, LANES), F32)],
        ins=(6,),
        hbm=(0, 1, 2, 3, 4, 5),
    )(
        contact_embedding, pairwise_final_matrix, edge_source_matrix, edge_target_matrix,
        edge_final_sigmoid_matrix, presence, zs[-1],
    )
    args = [y_msg, y_got, c_got, lefts, left_y, left_c, contact_t, live, w_o, w_p]
    first, gate, panels = call(
        functools.partial(pair_kernel, seqs=seqs, radix=radix, tile_rows=tile_rows, chans=chans),
        (pair, pair, shape((width, 2, tile_rows, cols), BF16)),
        [
            pltpu.VMEM((tile_rows, chans * chans, cols), BF16),
            pltpu.VMEM((LANES, cols), F32),
            pltpu.VMEM((2, width * tile_rows, cols), F32),
        ],
        ins=range(len(args)),
    )(*args)

    panels = lax.all_to_all(
        panels.reshape(devices, width // devices, 2, tile_rows, cols),
        ("rows", "cols"), split_axis=0, concat_axis=0, tiled=True,
    )
    product = call(
        functools.partial(triangle_kernel, n_rows=n_rows, n_cols=n_cols),
        shape((devices, width // devices, tile_rows, cols), BF16),
        [],
        ins=(0,),
    )(panels)
    product = lax.all_to_all(product, ("rows", "cols"), split_axis=0, concat_axis=0, tiled=True)
    return call(
        finish_kernel,
        jax.ShapeDtypeStruct((tile_rows, cols, pair_feats), F32),
        [
            pltpu.VMEM((width * tile_rows, cols), F32),
            pltpu.VMEM((tile_rows, cols, pair_feats), F32),
            pltpu.SemaphoreType.DMA((tile_rows // 2,)),
        ],
        ins=(0, 1, 2, 3, 4, 5),
        out_specs=pl.BlockSpec(memory_space=pl.ANY),
    )(
        product.reshape(width, tile_rows, cols), first, gate,
        edge_final_matrix.T, feedforward_expand_matrix.T, feedforward_shrink_matrix.T,
    )


def solution(mesh):
    tiles = P(("crops", "rows"), "cols", None)
    in_specs = (tiles, P(("crops", "rows"), "cols"), P("crops"), tiles) + (P(),) * 9

    return jax.shard_map(on_device, mesh=mesh, in_specs=in_specs, out_specs=tiles, check_vma=False)
```

```python
import functools

import jax
import jax.numpy as jnp
from jax import lax
from jax.experimental import pallas as pl
from jax.experimental.pallas import tpu as pltpu
from jax.sharding import PartitionSpec as P


EPS = 1e-05
F32 = jnp.float32
BF16 = jnp.bfloat16
TILE = 16
LANES = 128
VMEM_LIMIT = 32 * 2**20
PAD = 8
GROUP = 16
VMEM = pl.BlockSpec(memory_space=pltpu.VMEM)


def dot(a, b):
    return lax.dot_general(a, b, (((1,), (0,)), ((), ())), preferred_element_type=F32)


def dot_nt(a, b):
    return lax.dot_general(a, b, (((1,), (1,)), ((), ())), preferred_element_type=F32)


def sigmoid(x):
    return 0.5 * jnp.tanh(0.5 * x) + 0.5


def call(kernel, out_shape, scratch, ins=(), hbm=(), out_specs=None):
    def run(*args):
        args = [
            pltpu.with_memory_space_constraint(x, pltpu.VMEM if k in ins else pltpu.HBM)
            if k in ins or k in hbm
            else x
            for k, x in enumerate(args)
        ]
        return pl.pallas_call(
            kernel,
            out_shape=out_shape,
            in_specs=[VMEM] * len(args),
            out_specs=out_specs or jax.tree.map(lambda _: VMEM, out_shape),
            scratch_shapes=scratch,
            compiler_params=pltpu.CompilerParams(vmem_limit_bytes=VMEM_LIMIT),
        )(*args)

    return run


def project_kernel(fam_ref, keep_ref, pres_ref, wl_ref, wr_ref, right_ref, left_ref, nf, rs, *, tile_rows):
    seqs, cols, feats = fam_ref.shape
    chans = wl_ref.shape[0]
    col = lax.axis_index("cols")
    live = (keep_ref[...] * pres_ref[pl.ds(col, 1), :]).astype(F32)
    live_t = jnp.concatenate([live, jnp.zeros((LANES - seqs, cols), F32)], 0).T
    wr_t = wr_ref[...]
    for s in range(seqs):
        v = fam_ref[s]
        centred = v - jnp.mean(v, -1, keepdims=True)
        spread = jnp.mean(centred * centred, -1, keepdims=True)
        n = centred * (lax.rsqrt(spread + EPS) * live_t[:, s : s + 1])
        for h in range(feats // LANES):
            nf[h, pl.ds(s * (cols + PAD), cols), :] = n[:, h * LANES : (h + 1) * LANES]
        rs[pl.ds(s, chans, stride=seqs), :] = dot_nt(wr_t, n.astype(BF16))
    right_ref[0 : chans * seqs, :] = rs[...].astype(BF16)
    live_tile = jnp.concatenate([live, jnp.zeros((TILE - seqs, cols), F32)], 0).astype(BF16)
    right_ref[chans * seqs : chans * seqs + TILE, :] = live_tile
    per = LANES // chans
    groups = tile_rows // per
    pieces = cols // tile_rows
    wl = wl_ref[...].astype(F32).T
    acc = None
    for i4 in range(per):
        parts = []
        if i4:
            parts.append(jnp.zeros((feats, i4 * chans), F32))
        parts.append(wl)
        if i4 < per - 1:
            parts.append(jnp.zeros((feats, (per - 1 - i4) * chans), F32))
        w = jnp.concatenate(parts, 1).astype(BF16)
        rows = [
            jnp.concatenate(
                [nf[h, pl.ds(pq * per + i4, seqs, stride=cols + PAD), :] for h in range(feats // LANES)], 1
            )
            for pq in range(pieces * groups)
        ]
        part = dot(jnp.concatenate(rows, 0).astype(BF16), w)
        acc = part if acc is None else acc + part
    block = groups * seqs
    row = lax.axis_index("rows")
    planes = left_ref.shape[0]
    z, y, c = lax.rem(lax.div(row, 4), planes), lax.rem(lax.div(row, 2), 2), lax.rem(row, 2)
    for p in range(pieces):
        at = ((p // 4) ^ z, lax.rem((p // 2) % 2 + y, 2), lax.rem(p % 2 + c, 2))
        left_ref[at[0], at[1], at[2], 0:block, :] = acc[p * block : (p + 1) * block].astype(BF16)
        left_ref[at[0], at[1], at[2], block : block + TILE, :] = live_tile


def prepare_kernel(
    contact_ref, wo_ref, src_ref, tgt_ref, gate_ref, pres_ref, after_ref,
    contact_t_ref, wo_t_ref, wp_t_ref, live_ref,
    scr, column,
):
    tile_rows = contact_ref.shape[0]
    rows = wo_ref.shape[0]
    chans = int(rows**0.5)
    for i in range(tile_rows):
        contact_t_ref[i] = contact_ref[i].T
    scr[...] = wo_ref[...].astype(F32)
    for at in range(0, rows, LANES):
        part = jnp.concatenate(
            [scr[pl.ds(d, chans, stride=chans), :] for d in range(at // chans, (at + LANES) // chans)], 0
        )
        wo_t_ref[:, at : at + LANES] = part.T.astype(BF16)
    at = 0
    for ref in (src_ref, tgt_ref, gate_ref):
        wp_t_ref[at : at + ref.shape[1], :] = ref[...].astype(F32).T.astype(BF16)
        at += ref.shape[1]
    cols = contact_ref.shape[1]
    start = lax.axis_index("rows") * tile_rows
    live_i = pres_ref[pl.ds(lax.div(start, cols), 1), :].astype(F32)
    column[...] = jnp.broadcast_to(live_i, (LANES, cols)).T
    live_j = pres_ref[pl.ds(lax.axis_index("cols"), 1), :].astype(F32)
    live_ref[...] = column[pl.ds(pl.multiple_of(lax.rem(start, cols), 8), tile_rows), :] * live_j


def pair_kernel(
    z_ref, y_ref, c_ref, left_z_ref, left_y_ref, left_c_ref, contact_ref, live_ref, wo_ref, wp_ref,
    first_ref, gate_ref, panel_ref,
    o_scr, cnt_scr, pan_scr,
    *, seqs, radix, tile_rows, chans,
):
    right_rows, cols = z_ref.shape[0] // radix, z_ref.shape[1]
    tiles = right_rows // TILE - 1
    blocks = 4 * radix
    feats = first_ref.shape[1]
    pitch = tile_rows + PAD
    width = pan_scr.shape[1] // pitch
    pack = TILE // seqs
    per = LANES // chans
    groups = tile_rows // per
    row = lax.axis_index("rows")

    def right(b, t):
        core, pair, k = b // (2 * radix), b // radix % 2, b % radix
        ref, at = (c_ref, pair * radix + k) if core else (y_ref if pair else z_ref, k)
        return ref[at * right_rows + t * TILE : at * right_rows + (t + 1) * TILE, :]

    def left(b):
        core, pair, k = b // (2 * radix), b // radix % 2, b % radix
        if core:
            return left_c_ref[pair * radix + k]
        return left_y_ref[k, 0] if pair else left_z_ref[k, 0, 0]

    lefts = [left(b).astype(F32) for b in range(blocks)]
    block = groups * seqs
    live_l = jnp.concatenate([v[block : block + seqs] for v in lefts], 0).T.astype(BF16)
    live_r = jnp.concatenate([right(b, tiles).astype(F32)[:seqs] for b in range(blocks)], 0).astype(BF16)
    cnt_scr[...] = dot(live_l, live_r)
    start = lax.rem(row * tile_rows, cols)
    inv = 1.0 / jnp.maximum(cnt_scr[pl.ds(pl.multiple_of(start, 8), tile_rows), :], 1.0)
    zero = jnp.zeros((seqs, LANES), F32)
    ops = []
    for d2 in range(pack):
        for q in range(groups):
            rows = []
            for v in lefts:
                rows += [v[q * seqs : (q + 1) * seqs] if k == d2 else zero for k in range(pack)]
            ops.append(jnp.concatenate(rows, 0).T.astype(BF16))
    a_ext = jnp.concatenate(ops, 0)

    for t in range(0, tiles, 2):
        rhs = jnp.concatenate(
            [jnp.concatenate([right(b, u) for b in range(blocks)], 0) for u in (t, t + 1)], 1
        )
        out = dot(a_ext, rhs)
        for k in range(2):
            for d2 in range(pack):
                for i in range(tile_rows):
                    at = (d2 * tile_rows + i) * chans
                    val = out[at : at + chans, k * cols : (k + 1) * cols] * inv[i : i + 1]
                    d = (t + k) * pack + d2
                    o_scr[i, d * chans : (d + 1) * chans, :] = val.astype(BF16)

    w_o = wo_ref[...]
    w_p = wp_ref[...]
    for i in range(0, tile_rows, GROUP):
        upd = dot(w_o, jnp.concatenate([o_scr[i + k] for k in range(GROUP)], 1))
        normed = []
        for k in range(GROUP):
            first = contact_ref[i + k] + upd[:, k * cols : (k + 1) * cols]
            first_ref[i + k] = first
            centred = first - jnp.mean(first, 0, keepdims=True)
            spread = jnp.mean(centred * centred, 0, keepdims=True)
            normed.append((centred * lax.rsqrt(spread + EPS)).astype(BF16))
        raw = dot(w_p, jnp.concatenate(normed, 1))
        for k in range(GROUP):
            live = live_ref[i + k : i + k + 1, :]
            part = raw[:, k * cols : (k + 1) * cols]
            for side in range(2):
                at = side * 2 * width
                val = part[at : at + width] * sigmoid(part[at + width : at + 2 * width]) * live
                pan_scr[side, pl.ds(i + k, width, stride=pitch), :] = val
            gate_ref[i + k] = sigmoid(part[4 * width : 4 * width + feats])
    for ch in range(width):
        for side in range(2):
            panel_ref[ch, side] = pan_scr[side, ch * pitch : ch * pitch + tile_rows, :].astype(BF16)


def triangle_kernel(recv_ref, out_ref, *, n_rows, n_cols):
    own = recv_ref.shape[1]
    tile_rows, cols = recv_ref.shape[3:]
    for ch in range(own):
        sides = [
            jnp.concatenate(
                [
                    jnp.concatenate([recv_ref[r * n_cols + x, ch, side] for r in range(n_rows)], 0)
                    for x in range(n_cols)
                ],
                1,
            )
            for side in range(2)
        ]
        prod = dot_nt(sides[0], sides[1]).astype(BF16)
        for r in range(n_rows):
            for x in range(n_cols):
                out_ref[r * n_cols + x, ch] = prod[
                    r * tile_rows : (r + 1) * tile_rows, x * cols : (x + 1) * cols
                ]


def finish_kernel(prod_ref, first_ref, gate_ref, we_ref, w1_ref, w2_ref, hbm_ref, mix, out_ref, sems):
    chans, tile_rows, cols = prod_ref.shape
    pitch = tile_rows + PAD
    total = jnp.zeros((tile_rows, cols), F32)
    for ch in range(chans):
        total = total + prod_ref[ch].astype(F32)
    mean = total * (1.0 / chans)
    square = jnp.zeros((tile_rows, cols), F32)
    for ch in range(chans):
        centred = prod_ref[ch].astype(F32) - mean
        square = square + centred * centred
    scale = lax.rsqrt(square * (1.0 / chans) + EPS)
    for ch in range(chans):
        mix[ch * pitch : ch * pitch + tile_rows, :] = (prod_ref[ch].astype(F32) - mean) * scale
    w_e, w_1, w_2 = we_ref[...], w1_ref[...], w2_ref[...]
    copies = []
    for i in range(0, tile_rows, GROUP):
        mixed = jnp.concatenate(
            [mix[pl.ds(i + k, chans, stride=pitch), :].astype(BF16) for k in range(GROUP)], 1
        )
        proj = dot(w_e, mixed)
        seconds, normed = [], []
        for k in range(GROUP):
            second = first_ref[i + k] + gate_ref[i + k] * proj[:, k * cols : (k + 1) * cols]
            centred = second - jnp.mean(second, 0, keepdims=True)
            spread = jnp.mean(centred * centred, 0, keepdims=True)
            seconds.append(second)
            normed.append((centred * lax.rsqrt(spread + EPS)).astype(BF16))
        hidden = jnp.maximum(dot(w_1, jnp.concatenate(normed, 1)), 0.0).astype(BF16)
        out = dot(w_2, hidden)
        for k in range(GROUP):
            out_ref[i + k] = (seconds[k] + out[:, k * cols : (k + 1) * cols]).T
        copy = pltpu.make_async_copy(out_ref.at[pl.ds(i, GROUP)], hbm_ref.at[pl.ds(i, GROUP)], sems.at[i // GROUP])
        copy.start()
        copies.append(copy)
    for copy in copies:
        copy.wait()


def on_device(
    family_representation,
    family_keep_flags,
    amino_presence,
    contact_embedding,
    couple_lhs_weights,
    couple_rhs_weights,
    pairwise_final_matrix,
    edge_source_matrix,
    edge_target_matrix,
    edge_final_sigmoid_matrix,
    edge_final_matrix,
    feedforward_expand_matrix,
    feedforward_shrink_matrix,
):
    seqs, cols, feats = family_representation.shape
    tile_rows, _, pair_feats = contact_embedding.shape
    n_rows = lax.axis_size("rows")
    n_cols = lax.axis_size("cols")
    chans = couple_lhs_weights.shape[1]
    width = edge_source_matrix.shape[1] // 2
    devices = n_rows * n_cols
    radix = n_rows // 4
    pieces = cols // tile_rows
    col = lax.axis_index("cols")
    presence = amino_presence.reshape(n_cols, cols)
    shape = pltpu.VMEM
    planes = pieces // 4

    right_rows = chans * seqs + TILE
    left_rows = tile_rows * chans * seqs // LANES + TILE
    right, left = call(
        functools.partial(project_kernel, tile_rows=tile_rows),
        (shape((right_rows, cols), BF16), shape((pieces // 4, 2, 2, left_rows, LANES), BF16)),
        [pltpu.VMEM((feats // LANES, seqs * (cols + PAD), LANES), F32), pltpu.VMEM((chans * seqs, cols), F32)],
        hbm=(0, 1, 2, 3, 4),
    )(family_representation, family_keep_flags, presence, couple_lhs_weights.T, couple_rhs_weights.T)

    pair_y = [(i, i ^ 2) for i in range(n_rows)]
    pair_c = [(i, i ^ 1) for i in range(n_rows)]
    own = lax.axis_index("rows") // 4 // planes ^ col
    wide = jnp.zeros((n_cols,) + left.shape, BF16)
    wide = lax.dynamic_update_slice_in_dim(wide, left[None], own, 0)
    for k in range(1, n_cols):
        got = lax.ppermute(left, "cols", [(i, i ^ k) for i in range(n_cols)])
        wide = lax.dynamic_update_slice_in_dim(wide, got[None], own ^ k, 0)
    lefts = wide.reshape((1, radix) + left.shape[1:])
    y_msg = right
    half = radix // 2
    while half:
        pairs = [(i, i ^ (4 * half)) for i in range(n_rows)]
        y_msg = jnp.concatenate([y_msg, lax.ppermute(y_msg, "rows", pairs)], 0)
        lefts = jnp.concatenate([lefts[:, :half], lax.ppermute(lefts[:, half:], "rows", pairs)], 0)
        half //= 2
    lefts = lefts[:, 0]
    y_got = lax.ppermute(y_msg, "rows", pair_y)
    c_got = lax.ppermute(jnp.concatenate([y_msg, y_got], 0), "rows", pair_c)
    left_y = lax.ppermute(lefts[:, 1], "rows", pair_y)
    left_c = lax.ppermute(jnp.concatenate([lefts[:, 0, 1], left_y[:, 1]], 0), "rows", pair_c)

    pair = shape((tile_rows, pair_feats, cols), F32)
    contact_t, w_o, w_p, live = call(
        prepare_kernel,
        (
            pair,
            shape((pair_feats, chans * chans), BF16),
            shape((4 * width + pair_feats, pair_feats), BF16),
            shape((tile_rows, cols), F32),
        ),
        [pltpu.VMEM((chans * chans, pair_feats), F32), pltpu.VMEM((cols, LANES), F32)],
        ins=(6,),
        hbm=(0, 1, 2, 3, 4, 5),
    )(
        contact_embedding, pairwise_final_matrix, edge_source_matrix, edge_target_matrix,
        edge_final_sigmoid_matrix, presence, y_msg,
    )
    args = [y_msg, y_got, c_got, lefts, left_y, left_c, contact_t, live, w_o, w_p]
    first, gate, panels = call(
        functools.partial(pair_kernel, seqs=seqs, radix=radix, tile_rows=tile_rows, chans=chans),
        (pair, pair, shape((width, 2, tile_rows, cols), BF16)),
        [
            pltpu.VMEM((tile_rows, chans * chans, cols), BF16),
            pltpu.VMEM((LANES, cols), F32),
            pltpu.VMEM((2, width * (tile_rows + PAD), cols), F32),
        ],
        ins=range(len(args)),
    )(*args)

    panels = lax.all_to_all(
        panels.reshape(devices, width // devices, 2, tile_rows, cols),
        ("rows", "cols"), split_axis=0, concat_axis=0, tiled=True,
    )
    product = call(
        functools.partial(triangle_kernel, n_rows=n_rows, n_cols=n_cols),
        shape((devices, width // devices, tile_rows, cols), BF16),
        [],
        ins=(0,),
    )(panels)
    product = lax.all_to_all(product, ("rows", "cols"), split_axis=0, concat_axis=0, tiled=True)
    return call(
        finish_kernel,
        jax.ShapeDtypeStruct((tile_rows, cols, pair_feats), F32),
        [
            pltpu.VMEM((width * (tile_rows + PAD), cols), F32),
            pltpu.VMEM((tile_rows, cols, pair_feats), F32),
            pltpu.SemaphoreType.DMA((tile_rows // GROUP,)),
        ],
        ins=(0, 1, 2, 3, 4, 5),
        out_specs=pl.BlockSpec(memory_space=pl.ANY),
    )(
        product.reshape(width, tile_rows, cols), first, gate,
        edge_final_matrix.T, feedforward_expand_matrix.T, feedforward_shrink_matrix.T,
    )


def solution(mesh):
    tiles = P(("crops", "rows"), "cols", None)
    in_specs = (tiles, P(("crops", "rows"), "cols"), P("crops"), tiles) + (P(),) * 9

    return jax.shard_map(on_device, mesh=mesh, in_specs=in_specs, out_specs=tiles, check_vma=False)
```

```python
import functools

import jax
import jax.numpy as jnp
from jax import lax
from jax.experimental import pallas as pl
from jax.experimental.pallas import tpu as pltpu
from jax.sharding import PartitionSpec as P


EPS = 1e-05
F32 = jnp.float32
BF16 = jnp.bfloat16
TILE = 16
LANES = 128
VMEM_LIMIT = 32 * 2**20
PAD = 8
GROUP = 16
SEND = 4
VMEM = pl.BlockSpec(memory_space=pltpu.VMEM)


def dot(a, b):
    return lax.dot_general(a, b, (((1,), (0,)), ((), ())), preferred_element_type=F32)


def dot_nt(a, b):
    return lax.dot_general(a, b, (((1,), (1,)), ((), ())), preferred_element_type=F32)


def sigmoid(x):
    return 0.5 * jnp.tanh(0.5 * x) + 0.5


def call(kernel, out_shape, scratch, ins=(), hbm=(), out_specs=None):
    def run(*args):
        args = [
            pltpu.with_memory_space_constraint(x, pltpu.VMEM if k in ins else pltpu.HBM)
            if k in ins or k in hbm
            else x
            for k, x in enumerate(args)
        ]
        return pl.pallas_call(
            kernel,
            out_shape=out_shape,
            in_specs=[VMEM] * len(args),
            out_specs=out_specs or jax.tree.map(lambda _: VMEM, out_shape),
            scratch_shapes=scratch,
            compiler_params=pltpu.CompilerParams(vmem_limit_bytes=VMEM_LIMIT),
        )(*args)

    return run


def project_kernel(fam_ref, keep_ref, pres_ref, wl_ref, wr_ref, right_ref, left_ref, nf, rs, *, tile_rows):
    seqs, cols, feats = fam_ref.shape
    chans = wl_ref.shape[0]
    col = lax.axis_index("cols")
    live = (keep_ref[...] * pres_ref[pl.ds(col, 1), :]).astype(F32)
    live_t = jnp.concatenate([live, jnp.zeros((LANES - seqs, cols), F32)], 0).T
    wr_t = wr_ref[...]
    for s in range(seqs):
        v = fam_ref[s]
        centred = v - jnp.mean(v, -1, keepdims=True)
        spread = jnp.mean(centred * centred, -1, keepdims=True)
        n = centred * (lax.rsqrt(spread + EPS) * live_t[:, s : s + 1])
        for h in range(feats // LANES):
            nf[h, pl.ds(s * (cols + PAD), cols), :] = n[:, h * LANES : (h + 1) * LANES]
        rs[pl.ds(s, chans, stride=seqs), :] = dot_nt(wr_t, n.astype(BF16))
    right_ref[0 : chans * seqs, :] = rs[...].astype(BF16)
    live_tile = jnp.concatenate([live, jnp.zeros((TILE - seqs, cols), F32)], 0).astype(BF16)
    right_ref[chans * seqs : chans * seqs + TILE, :] = live_tile
    per = LANES // chans
    groups = tile_rows // per
    pieces = cols // tile_rows
    wl = wl_ref[...].astype(F32).T
    acc = None
    for i4 in range(per):
        parts = []
        if i4:
            parts.append(jnp.zeros((feats, i4 * chans), F32))
        parts.append(wl)
        if i4 < per - 1:
            parts.append(jnp.zeros((feats, (per - 1 - i4) * chans), F32))
        w = jnp.concatenate(parts, 1).astype(BF16)
        rows = [
            jnp.concatenate(
                [nf[h, pl.ds(pq * per + i4, seqs, stride=cols + PAD), :] for h in range(feats // LANES)], 1
            )
            for pq in range(pieces * groups)
        ]
        part = dot(jnp.concatenate(rows, 0).astype(BF16), w)
        acc = part if acc is None else acc + part
    block = groups * seqs
    row = lax.axis_index("rows")
    planes = left_ref.shape[0]
    z, y, c = lax.rem(lax.div(row, 4), planes), lax.rem(lax.div(row, 2), 2), lax.rem(row, 2)
    for p in range(pieces):
        at = ((p // 4) ^ z, lax.rem((p // 2) % 2 + y, 2), lax.rem(p % 2 + c, 2))
        left_ref[at[0], at[1], at[2], 0:block, :] = acc[p * block : (p + 1) * block].astype(BF16)
        left_ref[at[0], at[1], at[2], block : block + seqs, :] = live_tile[:seqs]


def prepare_kernel(
    contact_ref, wo_ref, src_ref, tgt_ref, gate_ref, pres_ref, after_ref,
    contact_t_ref, wo_t_ref, wp_t_ref, live_ref,
    scr, column,
):
    tile_rows = contact_ref.shape[0]
    rows = wo_ref.shape[0]
    chans = int(rows**0.5)
    for i in range(tile_rows):
        contact_t_ref[i] = contact_ref[i].T
    scr[...] = wo_ref[...].astype(F32)
    for at in range(0, rows, LANES):
        part = jnp.concatenate(
            [scr[pl.ds(d, chans, stride=chans), :] for d in range(at // chans, (at + LANES) // chans)], 0
        )
        wo_t_ref[:, at : at + LANES] = part.T.astype(BF16)
    at = 0
    for ref in (src_ref, tgt_ref, gate_ref):
        wp_t_ref[at : at + ref.shape[1], :] = ref[...].astype(F32).T.astype(BF16)
        at += ref.shape[1]
    cols = contact_ref.shape[1]
    start = lax.axis_index("rows") * tile_rows
    live_i = pres_ref[pl.ds(lax.div(start, cols), 1), :].astype(F32)
    column[...] = jnp.broadcast_to(live_i, (LANES, cols)).T
    live_j = pres_ref[pl.ds(lax.axis_index("cols"), 1), :].astype(F32)
    live_ref[...] = column[pl.ds(pl.multiple_of(lax.rem(start, cols), 8), tile_rows), :] * live_j


def pair_kernel(
    z_ref, y_ref, c_ref, left_z_ref, left_y_ref, left_c_ref, contact_ref, live_ref, wo_ref, wp_ref,
    first_ref, gate_ref, panel_ref,
    o_scr, cnt_scr, pan_scr,
    *, seqs, radix, tile_rows, chans,
):
    right_rows, cols = z_ref.shape[0] // radix, z_ref.shape[1]
    tiles = right_rows // TILE - 1
    blocks = 4 * radix
    feats = first_ref.shape[1]
    pitch = tile_rows + PAD
    width = pan_scr.shape[1] // pitch
    pack = TILE // seqs
    per = LANES // chans
    groups = tile_rows // per
    row = lax.axis_index("rows")

    def right(b, t):
        core, pair, k = b // (2 * radix), b // radix % 2, b % radix
        ref, at = (c_ref, pair * radix + k) if core else (y_ref if pair else z_ref, k)
        return ref[at * right_rows + t * TILE : at * right_rows + (t + 1) * TILE, :]

    def left(b):
        core, pair, k = b // (2 * radix), b // radix % 2, b % radix
        if core:
            return left_c_ref[pair * radix + k]
        return left_y_ref[k, 0] if pair else left_z_ref[k, 0, 0]

    lefts = [left(b).astype(F32) for b in range(blocks)]
    block = groups * seqs
    live_l = jnp.concatenate([v[block : block + seqs] for v in lefts], 0).T.astype(BF16)
    live_r = jnp.concatenate([right(b, tiles).astype(F32)[:seqs] for b in range(blocks)], 0).astype(BF16)
    cnt_scr[...] = dot(live_l, live_r)
    start = lax.rem(row * tile_rows, cols)
    inv = 1.0 / jnp.maximum(cnt_scr[pl.ds(pl.multiple_of(start, 8), tile_rows), :], 1.0)
    zero = jnp.zeros((seqs, LANES), F32)
    ops = []
    for d2 in range(pack):
        for q in range(groups):
            rows = []
            for v in lefts:
                rows += [v[q * seqs : (q + 1) * seqs] if k == d2 else zero for k in range(pack)]
            ops.append(jnp.concatenate(rows, 0).T.astype(BF16))
    a_ext = jnp.concatenate(ops, 0)

    for t in range(0, tiles, 2):
        rhs = jnp.concatenate(
            [jnp.concatenate([right(b, u) for b in range(blocks)], 0) for u in (t, t + 1)], 1
        )
        out = dot(a_ext, rhs)
        for k in range(2):
            for d2 in range(pack):
                for i in range(tile_rows):
                    at = (d2 * tile_rows + i) * chans
                    val = out[at : at + chans, k * cols : (k + 1) * cols] * inv[i : i + 1]
                    d = (t + k) * pack + d2
                    o_scr[i, d * chans : (d + 1) * chans, :] = val.astype(BF16)

    w_o = wo_ref[...]
    w_p = wp_ref[...]
    for i in range(0, tile_rows, GROUP):
        upd = dot(w_o, jnp.concatenate([o_scr[i + k] for k in range(GROUP)], 1))
        normed = []
        for k in range(GROUP):
            first = contact_ref[i + k] + upd[:, k * cols : (k + 1) * cols]
            first_ref[i + k] = first
            centred = first - jnp.mean(first, 0, keepdims=True)
            spread = jnp.mean(centred * centred, 0, keepdims=True)
            normed.append((centred * lax.rsqrt(spread + EPS)).astype(BF16))
        raw = dot(w_p, jnp.concatenate(normed, 1))
        for k in range(GROUP):
            live = live_ref[i + k : i + k + 1, :]
            part = raw[:, k * cols : (k + 1) * cols]
            for side in range(2):
                at = side * 2 * width
                val = part[at : at + width] * sigmoid(part[at + width : at + 2 * width]) * live
                pan_scr[side, pl.ds(i + k, width, stride=pitch), :] = val
            gate_ref[i + k] = sigmoid(part[4 * width : 4 * width + feats])
    for ch in range(width):
        for side in range(2):
            panel_ref[ch, side] = pan_scr[side, ch * pitch : ch * pitch + tile_rows, :].astype(BF16)


def triangle_kernel(recv_ref, out_ref, *, n_rows, n_cols):
    own = recv_ref.shape[1]
    tile_rows, cols = recv_ref.shape[3:]
    for ch in range(own):
        sides = [
            jnp.concatenate(
                [
                    jnp.concatenate([recv_ref[r * n_cols + x, ch, side] for r in range(n_rows)], 0)
                    for x in range(n_cols)
                ],
                1,
            )
            for side in range(2)
        ]
        prod = dot_nt(sides[0], sides[1]).astype(BF16)
        for r in range(n_rows):
            for x in range(n_cols):
                out_ref[r * n_cols + x, ch] = prod[
                    r * tile_rows : (r + 1) * tile_rows, x * cols : (x + 1) * cols
                ]


def finish_kernel(prod_ref, first_ref, gate_ref, we_ref, w1_ref, w2_ref, hbm_ref, mix, out_ref, sems):
    chans, tile_rows, cols = prod_ref.shape
    pitch = tile_rows + PAD
    total = jnp.zeros((tile_rows, cols), F32)
    for ch in range(chans):
        total = total + prod_ref[ch].astype(F32)
    mean = total * (1.0 / chans)
    square = jnp.zeros((tile_rows, cols), F32)
    for ch in range(chans):
        centred = prod_ref[ch].astype(F32) - mean
        square = square + centred * centred
    scale = lax.rsqrt(square * (1.0 / chans) + EPS)
    for ch in range(chans):
        mix[ch * pitch : ch * pitch + tile_rows, :] = (prod_ref[ch].astype(F32) - mean) * scale
    w_e, w_1, w_2 = we_ref[...], w1_ref[...], w2_ref[...]
    copies = []
    for i in range(0, tile_rows, GROUP):
        mixed = jnp.concatenate(
            [mix[pl.ds(i + k, chans, stride=pitch), :].astype(BF16) for k in range(GROUP)], 1
        )
        proj = dot(w_e, mixed)
        seconds, normed = [], []
        for k in range(GROUP):
            second = first_ref[i + k] + gate_ref[i + k] * proj[:, k * cols : (k + 1) * cols]
            centred = second - jnp.mean(second, 0, keepdims=True)
            spread = jnp.mean(centred * centred, 0, keepdims=True)
            seconds.append(second)
            normed.append((centred * lax.rsqrt(spread + EPS)).astype(BF16))
        hidden = jnp.maximum(dot(w_1, jnp.concatenate(normed, 1)), 0.0).astype(BF16)
        out = dot(w_2, hidden)
        for k in range(GROUP):
            out_ref[i + k] = (seconds[k] + out[:, k * cols : (k + 1) * cols]).T
            if (k + 1) % SEND == 0:
                part = pl.ds(i + k + 1 - SEND, SEND)
                copy = pltpu.make_async_copy(out_ref.at[part], hbm_ref.at[part], sems.at[(i + k) // SEND])
                copy.start()
                copies.append(copy)
    for copy in copies:
        copy.wait()


def on_device(
    family_representation,
    family_keep_flags,
    amino_presence,
    contact_embedding,
    couple_lhs_weights,
    couple_rhs_weights,
    pairwise_final_matrix,
    edge_source_matrix,
    edge_target_matrix,
    edge_final_sigmoid_matrix,
    edge_final_matrix,
    feedforward_expand_matrix,
    feedforward_shrink_matrix,
):
    seqs, cols, feats = family_representation.shape
    tile_rows, _, pair_feats = contact_embedding.shape
    n_rows = lax.axis_size("rows")
    n_cols = lax.axis_size("cols")
    chans = couple_lhs_weights.shape[1]
    width = edge_source_matrix.shape[1] // 2
    devices = n_rows * n_cols
    radix = n_rows // 4
    pieces = cols // tile_rows
    col = lax.axis_index("cols")
    presence = amino_presence.reshape(n_cols, cols)
    shape = pltpu.VMEM
    planes = pieces // 4

    right_rows = chans * seqs + TILE
    left_rows = tile_rows * chans * seqs // LANES + seqs
    right, left = call(
        functools.partial(project_kernel, tile_rows=tile_rows),
        (shape((right_rows, cols), BF16), shape((pieces // 4, 2, 2, left_rows, LANES), BF16)),
        [pltpu.VMEM((feats // LANES, seqs * (cols + PAD), LANES), F32), pltpu.VMEM((chans * seqs, cols), F32)],
        hbm=(0, 1, 2, 3, 4),
    )(family_representation, family_keep_flags, presence, couple_lhs_weights.T, couple_rhs_weights.T)

    pair_y = [(i, i ^ 2) for i in range(n_rows)]
    pair_c = [(i, i ^ 1) for i in range(n_rows)]
    own = lax.axis_index("rows") // 4 // planes ^ col
    wide = jnp.zeros((n_cols,) + left.shape, BF16)
    wide = lax.dynamic_update_slice_in_dim(wide, left[None], own, 0)
    for k in range(1, n_cols):
        got = lax.ppermute(left, "cols", [(i, i ^ k) for i in range(n_cols)])
        wide = lax.dynamic_update_slice_in_dim(wide, got[None], own ^ k, 0)
    lefts = wide.reshape((1, radix) + left.shape[1:])
    y_msg = right
    half = radix // 2
    while half:
        pairs = [(i, i ^ (4 * half)) for i in range(n_rows)]
        y_msg = jnp.concatenate([y_msg, lax.ppermute(y_msg, "rows", pairs)], 0)
        lefts = jnp.concatenate([lefts[:, :half], lax.ppermute(lefts[:, half:], "rows", pairs)], 0)
        half //= 2
    lefts = lefts[:, 0]
    y_got = lax.ppermute(y_msg, "rows", pair_y)
    c_got = lax.ppermute(jnp.concatenate([y_msg, y_got], 0), "rows", pair_c)
    left_y = lax.ppermute(lefts[:, 1], "rows", pair_y)
    left_c = lax.ppermute(jnp.concatenate([lefts[:, 0, 1], left_y[:, 1]], 0), "rows", pair_c)

    pair = shape((tile_rows, pair_feats, cols), F32)
    contact_t, w_o, w_p, live = call(
        prepare_kernel,
        (
            pair,
            shape((pair_feats, chans * chans), BF16),
            shape((4 * width + pair_feats, pair_feats), BF16),
            shape((tile_rows, cols), F32),
        ),
        [pltpu.VMEM((chans * chans, pair_feats), F32), pltpu.VMEM((cols, LANES), F32)],
        ins=(6,),
        hbm=(0, 1, 2, 3, 4, 5),
    )(
        contact_embedding, pairwise_final_matrix, edge_source_matrix, edge_target_matrix,
        edge_final_sigmoid_matrix, presence, y_msg,
    )
    args = [y_msg, y_got, c_got, lefts, left_y, left_c, contact_t, live, w_o, w_p]
    first, gate, panels = call(
        functools.partial(pair_kernel, seqs=seqs, radix=radix, tile_rows=tile_rows, chans=chans),
        (pair, pair, shape((width, 2, tile_rows, cols), BF16)),
        [
            pltpu.VMEM((tile_rows, chans * chans, cols), BF16),
            pltpu.VMEM((LANES, cols), F32),
            pltpu.VMEM((2, width * (tile_rows + PAD), cols), F32),
        ],
        ins=range(len(args)),
    )(*args)

    panels = lax.all_to_all(
        panels.reshape(devices, width // devices, 2, tile_rows, cols),
        ("rows", "cols"), split_axis=0, concat_axis=0, tiled=True,
    )
    product = call(
        functools.partial(triangle_kernel, n_rows=n_rows, n_cols=n_cols),
        shape((devices, width // devices, tile_rows, cols), BF16),
        [],
        ins=(0,),
    )(panels)
    product = lax.all_to_all(product, ("rows", "cols"), split_axis=0, concat_axis=0, tiled=True)
    return call(
        finish_kernel,
        jax.ShapeDtypeStruct((tile_rows, cols, pair_feats), F32),
        [
            pltpu.VMEM((width * (tile_rows + PAD), cols), F32),
            pltpu.VMEM((tile_rows, cols, pair_feats), F32),
            pltpu.SemaphoreType.DMA((tile_rows // SEND,)),
        ],
        ins=(0, 1, 2, 3, 4, 5),
        out_specs=pl.BlockSpec(memory_space=pl.ANY),
    )(
        product.reshape(width, tile_rows, cols), first, gate,
        edge_final_matrix.T, feedforward_expand_matrix.T, feedforward_shrink_matrix.T,
    )


def solution(mesh):
    tiles = P(("crops", "rows"), "cols", None)
    in_specs = (tiles, P(("crops", "rows"), "cols"), P("crops"), tiles) + (P(),) * 9

    return jax.shard_map(on_device, mesh=mesh, in_specs=in_specs, out_specs=tiles, check_vma=False)
```

```python
import functools

import jax
import jax.numpy as jnp
from jax import lax
from jax.experimental import pallas as pl
from jax.experimental.pallas import tpu as pltpu
from jax.sharding import PartitionSpec as P


EPS = 1e-05
F32 = jnp.float32
BF16 = jnp.bfloat16
TILE = 16
LANES = 128
VMEM_LIMIT = 32 * 2**20
PAD = 8
GROUP = 16
SEND = 4
VMEM = pl.BlockSpec(memory_space=pltpu.VMEM)


def dot(a, b):
    return lax.dot_general(a, b, (((1,), (0,)), ((), ())), preferred_element_type=F32)


def dot_nt(a, b):
    return lax.dot_general(a, b, (((1,), (1,)), ((), ())), preferred_element_type=F32)


def sigmoid(x):
    return 0.5 * jnp.tanh(0.5 * x) + 0.5


def call(kernel, out_shape, scratch, ins=(), hbm=(), out_specs=None):
    def run(*args):
        args = [
            pltpu.with_memory_space_constraint(x, pltpu.VMEM if k in ins else pltpu.HBM)
            if k in ins or k in hbm
            else x
            for k, x in enumerate(args)
        ]
        return pl.pallas_call(
            kernel,
            out_shape=out_shape,
            in_specs=[VMEM] * len(args),
            out_specs=out_specs or jax.tree.map(lambda _: VMEM, out_shape),
            scratch_shapes=scratch,
            compiler_params=pltpu.CompilerParams(vmem_limit_bytes=VMEM_LIMIT),
        )(*args)

    return run


def project_kernel(fam_ref, keep_ref, pres_ref, wl_ref, wr_ref, right_ref, left_ref, nf, rs, *, tile_rows):
    seqs, cols, feats = fam_ref.shape
    chans = wl_ref.shape[0]
    col = lax.axis_index("cols")
    live = (keep_ref[...] * pres_ref[pl.ds(col, 1), :]).astype(F32)
    live_t = jnp.concatenate([live, jnp.zeros((LANES - seqs, cols), F32)], 0).T
    wr_t = wr_ref[...]
    for s in range(seqs):
        v = fam_ref[s]
        centred = v - jnp.mean(v, -1, keepdims=True)
        spread = jnp.mean(centred * centred, -1, keepdims=True)
        n = centred * (lax.rsqrt(spread + EPS) * live_t[:, s : s + 1])
        for h in range(feats // LANES):
            nf[h, pl.ds(s * (cols + PAD), cols), :] = n[:, h * LANES : (h + 1) * LANES]
        rs[pl.ds(s, chans, stride=seqs), :] = dot_nt(wr_t, n.astype(BF16))
    right_ref[0 : chans * seqs, :] = rs[...].astype(BF16)
    live_tile = jnp.concatenate([live, jnp.zeros((TILE - seqs, cols), F32)], 0).astype(BF16)
    right_ref[chans * seqs : chans * seqs + TILE, :] = live_tile
    per = LANES // chans
    groups = tile_rows // per
    pieces = cols // tile_rows
    wl = wl_ref[...].astype(F32).T
    acc = None
    for i4 in range(per):
        parts = []
        if i4:
            parts.append(jnp.zeros((feats, i4 * chans), F32))
        parts.append(wl)
        if i4 < per - 1:
            parts.append(jnp.zeros((feats, (per - 1 - i4) * chans), F32))
        w = jnp.concatenate(parts, 1).astype(BF16)
        rows = [
            jnp.concatenate(
                [nf[h, pl.ds(pq * per + i4, seqs, stride=cols + PAD), :] for h in range(feats // LANES)], 1
            )
            for pq in range(pieces * groups)
        ]
        part = dot(jnp.concatenate(rows, 0).astype(BF16), w)
        acc = part if acc is None else acc + part
    block = groups * seqs
    row = lax.axis_index("rows")
    planes = left_ref.shape[0]
    z, y, c = lax.rem(lax.div(row, 4), planes), lax.rem(lax.div(row, 2), 2), lax.rem(row, 2)
    for p in range(pieces):
        at = ((p // 4) ^ z, lax.rem((p // 2) % 2 + y, 2), lax.rem(p % 2 + c, 2))
        left_ref[at[0], at[1], at[2], 0:block, :] = acc[p * block : (p + 1) * block].astype(BF16)
        left_ref[at[0], at[1], at[2], block : block + seqs, :] = live_tile[:seqs]


def prepare_kernel(
    contact_ref, wo_ref, src_ref, tgt_ref, gate_ref, pres_ref, after_ref,
    contact_t_ref, wo_t_ref, wp_t_ref, live_ref,
    scr, column,
):
    tile_rows = contact_ref.shape[0]
    rows = wo_ref.shape[0]
    chans = int(rows**0.5)
    for i in range(tile_rows):
        contact_t_ref[i] = contact_ref[i].T
    scr[...] = wo_ref[...].astype(F32)
    for at in range(0, rows, LANES):
        part = jnp.concatenate(
            [scr[pl.ds(d, chans, stride=chans), :] for d in range(at // chans, (at + LANES) // chans)], 0
        )
        wo_t_ref[:, at : at + LANES] = part.T.astype(BF16)
    at = 0
    for ref in (src_ref, tgt_ref, gate_ref):
        wp_t_ref[at : at + ref.shape[1], :] = ref[...].astype(F32).T.astype(BF16)
        at += ref.shape[1]
    cols = contact_ref.shape[1]
    start = lax.axis_index("rows") * tile_rows
    live_i = pres_ref[pl.ds(lax.div(start, cols), 1), :].astype(F32)
    column[...] = jnp.broadcast_to(live_i, (LANES, cols)).T
    live_j = pres_ref[pl.ds(lax.axis_index("cols"), 1), :].astype(F32)
    live_ref[...] = column[pl.ds(pl.multiple_of(lax.rem(start, cols), 8), tile_rows), :] * live_j


def pair_kernel(
    z_ref, y_ref, c_first_ref, c_last_ref, left_z_ref, left_y_ref, left_c_ref, contact_ref, live_ref, wo_ref, wp_ref,
    first_ref, gate_ref, panel_ref,
    o_scr, cnt_scr, pan_scr,
    *, seqs, radix, tile_rows, chans,
):
    right_rows, cols = z_ref.shape[0] // radix, z_ref.shape[1]
    tiles = right_rows // TILE - 1
    blocks = 4 * radix
    feats = first_ref.shape[1]
    pitch = tile_rows + PAD
    width = pan_scr.shape[1] // pitch
    pack = TILE // seqs
    per = LANES // chans
    groups = tile_rows // per
    row = lax.axis_index("rows")

    def right(b, t):
        core, pair, k = b // (2 * radix), b // radix % 2, b % radix
        ref = ((z_ref, y_ref), (c_first_ref, c_last_ref))[core][pair]
        return ref[k * right_rows + t * TILE : k * right_rows + (t + 1) * TILE, :]

    def left(b):
        core, pair, k = b // (2 * radix), b // radix % 2, b % radix
        if core:
            return left_c_ref[pair * radix + k]
        return left_y_ref[k, 0] if pair else left_z_ref[k, 0, 0]

    lefts = [left(b).astype(F32) for b in range(blocks)]
    block = groups * seqs
    live_l = jnp.concatenate([v[block : block + seqs] for v in lefts], 0).T.astype(BF16)
    live_r = jnp.concatenate([right(b, tiles).astype(F32)[:seqs] for b in range(blocks)], 0).astype(BF16)
    cnt_scr[...] = dot(live_l, live_r)
    start = lax.rem(row * tile_rows, cols)
    inv = 1.0 / jnp.maximum(cnt_scr[pl.ds(pl.multiple_of(start, 8), tile_rows), :], 1.0)
    zero = jnp.zeros((seqs, LANES), F32)
    ops = []
    for d2 in range(pack):
        for q in range(groups):
            rows = []
            for v in lefts:
                rows += [v[q * seqs : (q + 1) * seqs] if k == d2 else zero for k in range(pack)]
            ops.append(jnp.concatenate(rows, 0).T.astype(BF16))
    a_ext = jnp.concatenate(ops, 0)

    for t in range(0, tiles, 2):
        rhs = jnp.concatenate(
            [jnp.concatenate([right(b, u) for b in range(blocks)], 0) for u in (t, t + 1)], 1
        )
        out = dot(a_ext, rhs)
        for k in range(2):
            for d2 in range(pack):
                for i in range(tile_rows):
                    at = (d2 * tile_rows + i) * chans
                    val = out[at : at + chans, k * cols : (k + 1) * cols] * inv[i : i + 1]
                    d = (t + k) * pack + d2
                    o_scr[i, d * chans : (d + 1) * chans, :] = val.astype(BF16)

    w_o = wo_ref[...]
    w_p = wp_ref[...]
    for i in range(0, tile_rows, GROUP):
        upd = dot(w_o, jnp.concatenate([o_scr[i + k] for k in range(GROUP)], 1))
        normed = []
        for k in range(GROUP):
            first = contact_ref[i + k] + upd[:, k * cols : (k + 1) * cols]
            first_ref[i + k] = first
            centred = first - jnp.mean(first, 0, keepdims=True)
            spread = jnp.mean(centred * centred, 0, keepdims=True)
            normed.append((centred * lax.rsqrt(spread + EPS)).astype(BF16))
        raw = dot(w_p, jnp.concatenate(normed, 1))
        for k in range(GROUP):
            live = live_ref[i + k : i + k + 1, :]
            part = raw[:, k * cols : (k + 1) * cols]
            for side in range(2):
                at = side * 2 * width
                val = part[at : at + width] * sigmoid(part[at + width : at + 2 * width]) * live
                pan_scr[side, pl.ds(i + k, width, stride=pitch), :] = val
            gate_ref[i + k] = sigmoid(part[4 * width : 4 * width + feats])
    for ch in range(width):
        for side in range(2):
            panel_ref[ch, side] = pan_scr[side, ch * pitch : ch * pitch + tile_rows, :].astype(BF16)


def triangle_kernel(recv_ref, out_ref, *, n_rows, n_cols):
    own = recv_ref.shape[1]
    tile_rows, cols = recv_ref.shape[3:]
    for ch in range(own):
        sides = [
            jnp.concatenate(
                [
                    jnp.concatenate([recv_ref[r * n_cols + x, ch, side] for r in range(n_rows)], 0)
                    for x in range(n_cols)
                ],
                1,
            )
            for side in range(2)
        ]
        prod = dot_nt(sides[0], sides[1]).astype(BF16)
        for r in range(n_rows):
            for x in range(n_cols):
                out_ref[r * n_cols + x, ch] = prod[
                    r * tile_rows : (r + 1) * tile_rows, x * cols : (x + 1) * cols
                ]


def finish_kernel(prod_ref, first_ref, gate_ref, we_ref, w1_ref, w2_ref, hbm_ref, mix, out_ref, sems):
    chans, tile_rows, cols = prod_ref.shape
    pitch = tile_rows + PAD
    total = jnp.zeros((tile_rows, cols), F32)
    for ch in range(chans):
        total = total + prod_ref[ch].astype(F32)
    mean = total * (1.0 / chans)
    square = jnp.zeros((tile_rows, cols), F32)
    for ch in range(chans):
        centred = prod_ref[ch].astype(F32) - mean
        square = square + centred * centred
    scale = lax.rsqrt(square * (1.0 / chans) + EPS)
    for ch in range(chans):
        mix[ch * pitch : ch * pitch + tile_rows, :] = (prod_ref[ch].astype(F32) - mean) * scale
    w_e, w_1, w_2 = we_ref[...], w1_ref[...], w2_ref[...]
    copies = []
    for i in range(0, tile_rows, GROUP):
        mixed = jnp.concatenate(
            [mix[pl.ds(i + k, chans, stride=pitch), :].astype(BF16) for k in range(GROUP)], 1
        )
        proj = dot(w_e, mixed)
        seconds, normed = [], []
        for k in range(GROUP):
            second = first_ref[i + k] + gate_ref[i + k] * proj[:, k * cols : (k + 1) * cols]
            centred = second - jnp.mean(second, 0, keepdims=True)
            spread = jnp.mean(centred * centred, 0, keepdims=True)
            seconds.append(second)
            normed.append((centred * lax.rsqrt(spread + EPS)).astype(BF16))
        hidden = jnp.maximum(dot(w_1, jnp.concatenate(normed, 1)), 0.0).astype(BF16)
        out = dot(w_2, hidden)
        for k in range(GROUP):
            out_ref[i + k] = (seconds[k] + out[:, k * cols : (k + 1) * cols]).T
            if (k + 1) % SEND == 0:
                part = pl.ds(i + k + 1 - SEND, SEND)
                copy = pltpu.make_async_copy(out_ref.at[part], hbm_ref.at[part], sems.at[(i + k) // SEND])
                copy.start()
                copies.append(copy)
    for copy in copies:
        copy.wait()


def on_device(
    family_representation,
    family_keep_flags,
    amino_presence,
    contact_embedding,
    couple_lhs_weights,
    couple_rhs_weights,
    pairwise_final_matrix,
    edge_source_matrix,
    edge_target_matrix,
    edge_final_sigmoid_matrix,
    edge_final_matrix,
    feedforward_expand_matrix,
    feedforward_shrink_matrix,
):
    seqs, cols, feats = family_representation.shape
    tile_rows, _, pair_feats = contact_embedding.shape
    n_rows = lax.axis_size("rows")
    n_cols = lax.axis_size("cols")
    chans = couple_lhs_weights.shape[1]
    width = edge_source_matrix.shape[1] // 2
    devices = n_rows * n_cols
    radix = n_rows // 4
    pieces = cols // tile_rows
    col = lax.axis_index("cols")
    presence = amino_presence.reshape(n_cols, cols)
    shape = pltpu.VMEM
    planes = pieces // 4

    right_rows = chans * seqs + TILE
    left_rows = tile_rows * chans * seqs // LANES + seqs
    right, left = call(
        functools.partial(project_kernel, tile_rows=tile_rows),
        (shape((right_rows, cols), BF16), shape((pieces // 4, 2, 2, left_rows, LANES), BF16)),
        [pltpu.VMEM((feats // LANES, seqs * (cols + PAD), LANES), F32), pltpu.VMEM((chans * seqs, cols), F32)],
        hbm=(0, 1, 2, 3, 4),
    )(family_representation, family_keep_flags, presence, couple_lhs_weights.T, couple_rhs_weights.T)

    pair_y = [(i, i ^ 2) for i in range(n_rows)]
    pair_c = [(i, i ^ 1) for i in range(n_rows)]
    own = lax.axis_index("rows") // 4 // planes ^ col
    wide = jnp.zeros((n_cols,) + left.shape, BF16)
    wide = lax.dynamic_update_slice_in_dim(wide, left[None], own, 0)
    for k in range(1, n_cols):
        got = lax.ppermute(left, "cols", [(i, i ^ k) for i in range(n_cols)])
        wide = lax.dynamic_update_slice_in_dim(wide, got[None], own ^ k, 0)
    lefts = wide.reshape((1, radix) + left.shape[1:])
    y_msg = right
    half = radix // 2
    while half:
        pairs = [(i, i ^ (4 * half)) for i in range(n_rows)]
        y_msg = jnp.concatenate([y_msg, lax.ppermute(y_msg, "rows", pairs)], 0)
        lefts = jnp.concatenate([lefts[:, :half], lax.ppermute(lefts[:, half:], "rows", pairs)], 0)
        half //= 2
    lefts = lefts[:, 0]
    y_got = lax.ppermute(y_msg, "rows", pair_y)
    c_first = lax.ppermute(y_msg, "rows", pair_c)
    c_last = lax.ppermute(y_got, "rows", pair_c)
    left_y = lax.ppermute(lefts[:, 1], "rows", pair_y)
    left_c = lax.ppermute(jnp.concatenate([lefts[:, 0, 1], left_y[:, 1]], 0), "rows", pair_c)

    pair = shape((tile_rows, pair_feats, cols), F32)
    contact_t, w_o, w_p, live = call(
        prepare_kernel,
        (
            pair,
            shape((pair_feats, chans * chans), BF16),
            shape((4 * width + pair_feats, pair_feats), BF16),
            shape((tile_rows, cols), F32),
        ),
        [pltpu.VMEM((chans * chans, pair_feats), F32), pltpu.VMEM((cols, LANES), F32)],
        ins=(6,),
        hbm=(0, 1, 2, 3, 4, 5),
    )(
        contact_embedding, pairwise_final_matrix, edge_source_matrix, edge_target_matrix,
        edge_final_sigmoid_matrix, presence, y_msg,
    )
    args = [y_msg, y_got, c_first, c_last, lefts, left_y, left_c, contact_t, live, w_o, w_p]
    first, gate, panels = call(
        functools.partial(pair_kernel, seqs=seqs, radix=radix, tile_rows=tile_rows, chans=chans),
        (pair, pair, shape((width, 2, tile_rows, cols), BF16)),
        [
            pltpu.VMEM((tile_rows, chans * chans, cols), BF16),
            pltpu.VMEM((LANES, cols), F32),
            pltpu.VMEM((2, width * (tile_rows + PAD), cols), F32),
        ],
        ins=range(len(args)),
    )(*args)

    panels = lax.all_to_all(
        panels.reshape(devices, width // devices, 2, tile_rows, cols),
        ("rows", "cols"), split_axis=0, concat_axis=0, tiled=True,
    )
    product = call(
        functools.partial(triangle_kernel, n_rows=n_rows, n_cols=n_cols),
        shape((devices, width // devices, tile_rows, cols), BF16),
        [],
        ins=(0,),
    )(panels)
    product = lax.all_to_all(product, ("rows", "cols"), split_axis=0, concat_axis=0, tiled=True)
    return call(
        finish_kernel,
        jax.ShapeDtypeStruct((tile_rows, cols, pair_feats), F32),
        [
            pltpu.VMEM((width * (tile_rows + PAD), cols), F32),
            pltpu.VMEM((tile_rows, cols, pair_feats), F32),
            pltpu.SemaphoreType.DMA((tile_rows // SEND,)),
        ],
        ins=(0, 1, 2, 3, 4, 5),
        out_specs=pl.BlockSpec(memory_space=pl.ANY),
    )(
        product.reshape(width, tile_rows, cols), first, gate,
        edge_final_matrix.T, feedforward_expand_matrix.T, feedforward_shrink_matrix.T,
    )


def solution(mesh):
    tiles = P(("crops", "rows"), "cols", None)
    in_specs = (tiles, P(("crops", "rows"), "cols"), P("crops"), tiles) + (P(),) * 9

    return jax.shard_map(on_device, mesh=mesh, in_specs=in_specs, out_specs=tiles, check_vma=False)
```
